16 devices in a mesh: rep: 1, dp: 16 (over x, y, z, core).
Axes of the slice: x: 2, y: 2, z: 2, core: 2. Of those that a mesh axis runs over, the one named last changes fastest.
Arguments:
- x: bfloat16 [16, 2048, 1280], P(('rep', 'dp'))
- dy: bfloat16 [16, 2048, 1280], P(('rep', 'dp'))
- w_gate: bfloat16 [2, 1280, 3072], P(None, 'dp')
- w_up: bfloat16 [2, 1280, 3072], P(None, 'dp')
- w_down: bfloat16 [2, 3072, 1280], P(None, 'dp')
- m_w_gate: float32 [2, 1280, 3072], P(None, 'dp')
- m_w_up: float32 [2, 1280, 3072], P(None, 'dp')
- m_w_down: float32 [2, 3072, 1280], P(None, 'dp')
- v_w_gate: float32 [2, 1280, 3072], P(None, 'dp')
- v_w_up: float32 [2, 1280, 3072], P(None, 'dp')
- v_w_down: float32 [2, 3072, 1280], P(None, 'dp')
Outputs:
- output 1: bfloat16 [2, 1280, 3072], P('rep', 'dp')
- output 2: bfloat16 [2, 1280, 3072], P('rep', 'dp')
- output 3: bfloat16 [2, 3072, 1280], P('rep', 'dp')
- output 4: float32 [2, 1280, 3072], P('rep', 'dp')
- output 5: float32 [2, 1280, 3072], P('rep', 'dp')
- output 6: float32 [2, 3072, 1280], P('rep', 'dp')
- output 7: float32 [2, 1280, 3072], P('rep', 'dp')
- output 8: float32 [2, 1280, 3072], P('rep', 'dp')
- output 9: float32 [2, 3072, 1280], P('rep', 'dp')
All inputs are finite; a program needn't handle non-finite values.
Results may differ from the reference program's by a relative error of at most 0.022.
Values are sent between devices in bfloat16 or wider.
A program may use at most 2 GiB of HBM per device.

```python
import jax
import jax.numpy as jnp
from jax import lax

SEQUENCES = 16
TOKENS = 2048
D = 1280
FF = 3072
LAYERS = 2
NAMES = ("w_gate", "w_up", "w_down")
SHAPES = {"w_gate": (LAYERS, D, FF), "w_up": (LAYERS, D, FF), "w_down": (LAYERS, FF, D)}


def bump(key, n, height):
    away = (jnp.arange(n, dtype=jnp.int32) - jax.random.randint(key, (), 0, n, jnp.int32)) % n
    return jnp.where(away < n // 8, height, 1.0)


def together(key, own, strength):
    shared = jax.random.normal(key, own.shape[1:], jnp.float32)
    return (own + strength * shared) * lax.rsqrt(1 + strength * strength)


def setup_inputs(seed: int = 0, part: int = 0) -> dict:
    kx, kdy, ka, kb, kz, kf, kh, kl, *keys = jax.random.split(jax.random.key(seed), 8 + 3 * len(NAMES))
    kx, kdy, ka, kb = (jax.random.fold_in(k, part) for k in (kx, kdy, ka, kb))
    kw, km, kv = (keys[i::3] for i in range(3))
    shape = (SEQUENCES, TOKENS, D)
    much_x, much_dy = jax.random.uniform(kz, (2,), jnp.float32, 0.0, 1.0)
    loud = 2.0 ** jax.random.uniform(jax.random.fold_in(kz, 1), (), jnp.float32, -1.0, 2.0)
    layers = 2.0 ** jax.random.uniform(kl, (LAYERS, 1, 1), jnp.float32, -1.0, 1.0)
    x = together(ka, jax.random.normal(kx, shape, jnp.float32), much_x) * bump(kf, D, 4.0)
    dy = together(kb, jax.random.normal(kdy, shape, jnp.float32), much_dy)
    drawn = {"x": x.astype(jnp.bfloat16), "dy": (loud * dy * (SEQUENCES * TOKENS) ** -0.5).astype(jnp.bfloat16)}
    for key, name in zip(kw, NAMES, strict=True):
        w = jax.random.normal(key, SHAPES[name], jnp.float32) * SHAPES[name][1] ** -0.5
        drawn[name] = (w * {"w_gate": 1.0, "w_up": bump(kh, FF, 4.0), "w_down": layers}[name]).astype(jnp.bfloat16)
    for key, name in zip(km, NAMES, strict=True):
        drawn[f"m_{name}"] = 0.1 * jax.random.normal(key, SHAPES[name], jnp.float32)
    for key, name in zip(kv, NAMES, strict=True):
        drawn[f"v_{name}"] = jax.random.uniform(key, SHAPES[name], jnp.float32, 0.005, 0.015)
    return drawn


def matmul(a, w):
    return jnp.dot(a, w, preferred_element_type=jnp.float32).astype(jnp.bfloat16)


def normed(h):
    wide = h.astype(jnp.float32)
    scale = lax.rsqrt(jnp.mean(wide**2, -1, keepdims=True) + 1e-6)
    return (wide * scale).astype(jnp.bfloat16)


def layer(h, w):
    a = normed(h)
    gate = jnp.dot(a, w["w_gate"], preferred_element_type=jnp.float32)
    up = jnp.dot(a, w["w_up"], preferred_element_type=jnp.float32)
    return h + matmul((jax.nn.silu(gate) * up).astype(jnp.bfloat16), w["w_down"])


def adamw(w, m, v, g):
    m = 0.9 * m + 0.1 * g
    v = 0.95 * v + 0.05 * g * g
    step = m * lax.rsqrt(v + 1e-8) + 0.1 * w
    return (w - 0.02 * step).astype(jnp.bfloat16), m, v


def clipped(gradients, sum_of_squares, count):
    factor = jnp.minimum(1.0, 0.5 * lax.rsqrt(sum_of_squares / count + 1e-30))
    return [g * factor for g in gradients]


def stack(weights, h):
    return lax.scan(lambda h, w: (layer(h, w), None), h, weights)[0]


def reference(x, dy, w_gate, w_up, w_down, m_w_gate, m_w_up, m_w_down, v_w_gate, v_w_up, v_w_down):
    weights = dict(zip(NAMES, (w_gate, w_up, w_down), strict=True))

    def take(so_far, sequence):
        h, by_y = sequence
        _, back = jax.vjp(lambda w: stack(w, h), weights)
        return jax.tree.map(lambda total, term: total + term.astype(jnp.float32), so_far, back(by_y)[0]), None

    none_yet = {name: jnp.zeros(w.shape, jnp.float32) for name, w in weights.items()}
    by_weights, _ = lax.scan(take, none_yet, (x, dy))
    gradients = [by_weights[name].astype(jnp.bfloat16).astype(jnp.float32) for name in NAMES]
    gradients = clipped(gradients, sum(jnp.sum(g * g) for g in gradients), sum(g.size for g in gradients))
    new = [
        adamw(w.astype(jnp.float32), m, v, g)
        for w, m, v, g in zip((w_gate, w_up, w_down), (m_w_gate, m_w_up, m_w_down), (v_w_gate, v_w_up, v_w_down), gradients, strict=True)
    ]
    return tuple(one[which] for which in range(3) for one in new)
```

```python
import functools

import jax
import jax.numpy as jnp
from jax import lax
from jax.experimental import pallas as pl
from jax.experimental.pallas import tpu as pltpu
from jax.sharding import PartitionSpec as P

MESH = pl.DeviceIdType.MESH
F32, BF16 = jnp.float32, jnp.bfloat16
ANY = pl.BlockSpec(memory_space=pl.ANY)
AXES = (8, 4, 2)
TURNS = ((8, 4, 2), (4, 2, 8), (2, 8, 4))
TOKENS, D, FF = 2048, 1280, 3072
TILE = 256


class Here:
    def __init__(self):
        me = lax.axis_index("dp")
        self.me = me
        self.bit = {b: lax.rem(lax.div(me, b), 2) for b in (8, 4, 2, 1)}

    def peer(self, b):
        return {"dp": self.me + b * (1 - 2 * self.bit[b])}

    def at(self, how):
        out = []
        for b, h in how:
            out.append(self.bit[b] if h == "m" else 1 - self.bit[b] if h == "o" else slice(None))
        return tuple(out)


def send(src, dst, sems, i, device):
    return pltpu.make_async_remote_copy(
        src_ref=src, dst_ref=dst, send_sem=sems.at[0, i], recv_sem=sems.at[1, i], device_id=device, device_id_type=MESH
    )


def pieces(rows, cols):
    if cols == FF:
        third, half = FF // 3, FF // 6
        return [[(slice(0, rows), slice(r * third + h * half, r * third + (h + 1) * half)) for r in range(3)] for h in range(2)]
    third, half = rows // 3, cols // 2
    return [[(slice(r * third, (r + 1) * third), slice(h * half, (h + 1) * half)) for r in range(3)] for h in range(2)]


class Gather:
    peers = (8, 4, 2, 1)
    n_in = n_out = 1

    def __init__(self, blocks, layer, lag=0.0):
        self.array = blocks
        self.rows, self.cols = blocks.shape[1:]
        self.layer, self.lag = layer, lag

    def inputs(self):
        layer = self.layer
        return [(self.array, pl.BlockSpec((1, self.rows, self.cols), lambda *_: (layer, 0, 0)))]

    def outputs(self):
        return [(jax.ShapeDtypeStruct((2, 2, 2, 2, self.rows, self.cols), BF16), ANY)]

    def scratch(self):
        return [pltpu.SemaphoreType.DMA((2, 18)), pltpu.SemaphoreType.DMA((2, 19)), pltpu.SemaphoreType.DMA]

    def events(self, here, ins, outs, scratch):
        (own,), (full,), (wire, cores, local) = ins, outs, scratch
        own = own.at[0]
        parts = pieces(self.rows, self.cols)
        mine = here.at([(b, "m") for b in (8, 4, 2, 1)])

        def view(how, h, r):
            return full.at[here.at([(b, how.get(b, "m")) for b in (8, 4, 2, 1)]) + parts[h][r]]

        def hop(p, h, r):
            d = TURNS[r]
            src = view({b: "f" for b in d[:p]}, h, r)
            dst = src
            if p == 0:
                src = own.at[parts[h][r]]
            return send(src, dst, wire, (p * 2 + h) * 3 + r, here.peer(d[p]))

        def across(p, h, r):
            d = TURNS[r]
            ref = view({**{b: "f" for b in d[:p]}, d[p]: "o"}, h, r)
            return send(ref, ref, cores, (p * 2 + h) * 3 + r, here.peer(1))

        def own_across():
            return send(own, full.at[mine], cores, 18, here.peer(1))

        keep = pltpu.make_async_copy(own, full.at[mine], local)

        def begin():
            for h in range(2):
                for r in range(3):
                    hop(0, h, r).start()
            keep.start()
            own_across().start()
            keep.wait()

        def onward(p, h):
            for r in range(3):
                hop(p, h, r).wait_recv()
                if p < 2:
                    hop(p + 1, h, r).start()
                across(p, h, r).start()

        def finish():
            for p in range(3):
                for h in range(2):
                    for r in range(3):
                        hop(p, h, r).wait_send()
                        across(p, h, r).wait()
            own_across().wait()

        times = {(0, 0): 4.0, (0, 1): 5.8, (1, 0): 9.5, (1, 1): 13.0, (2, 0): 20.0, (2, 1): 27.0}
        out = [(self.lag, begin)]
        for (p, h), t in times.items():
            out.append((self.lag + t, functools.partial(onward, p, h)))
        out.append((1e9, finish))
        return out


class Scatter:
    peers = (8, 4, 2)
    n_in = n_out = 1

    def __init__(self, sums, lag=0.0):
        self.array = sums
        self.rows, self.cols = sums.shape[3:]
        self.lag = lag

    def inputs(self):
        return [(self.array, ANY)]

    def outputs(self):
        return [(jax.ShapeDtypeStruct((self.rows, self.cols), BF16), pl.BlockSpec((self.rows, self.cols), lambda *_: (0, 0)))]

    def scratch(self):
        r, c = pieces(self.rows, self.cols)[0][0]
        r, c = r.stop - r.start, c.stop - c.start
        legs = [pltpu.VMEM((6, *lead, r, c), BF16) for lead in ((2, 2), (2,), ())]
        return [pltpu.VMEM((2, 2, 2, self.rows, self.cols), F32), *legs, *legs, pltpu.SemaphoreType.DMA((2, 18)), pltpu.SemaphoreType.DMA]

    def events(self, here, ins, outs, scratch):
        (sums,), (out,) = ins, outs
        held, *legs, wire, local = scratch
        going, coming = legs[:3], legs[3:]
        parts = pieces(self.rows, self.cols)
        load = pltpu.make_async_copy(sums, held, local)

        def place(order, picks):
            where = dict(zip(order, picks, strict=True))
            return tuple(where[b] for b in AXES)

        def hop(p, h, r):
            q = h * 3 + r
            return send(going[p].at[q], coming[p].at[q], wire, p * 6 + q, here.peer(TURNS[r][p]))

        def begin():
            load.start()

        def first(h):
            if h == 0:
                load.wait()
            for r in range(3):
                d, q = TURNS[r], h * 3 + r
                for i in range(2):
                    for j in range(2):
                        going[0][q, i, j] = held[place(d, (1 - here.bit[d[0]], i, j)) + parts[h][r]].astype(BF16)
                hop(0, h, r).start()

        def onward(p, h):
            for r in range(3):
                d, q = TURNS[r], h * 3 + r
                mine = [here.bit[b] for b in d]
                hop(p, h, r).wait_recv()
                if p == 0:
                    for j in range(2):
                        at = place(d, (mine[0], 1 - mine[1], j)) + parts[h][r]
                        going[1][q, j] = (held[at] + coming[0][q, 1 - mine[1], j].astype(F32)).astype(BF16)
                    hop(1, h, r).start()
                    for j in range(2):
                        at = place(d, (mine[0], mine[1], j)) + parts[h][r]
                        held[at] = held[at] + coming[0][q, mine[1], j].astype(F32)
                elif p == 1:
                    at = place(d, (mine[0], mine[1], 1 - mine[2])) + parts[h][r]
                    going[2][q] = (held[at] + coming[1][q, 1 - mine[2]].astype(F32)).astype(BF16)
                    hop(2, h, r).start()
                    at = place(d, mine) + parts[h][r]
                    held[at] = held[at] + coming[1][q, mine[2]].astype(F32)
                else:
                    at = place(d, mine) + parts[h][r]
                    out[parts[h][r]] = (held[at] + coming[2][q].astype(F32)).astype(BF16)

        def finish():
            for p in range(3):
                for h in range(2):
                    for r in range(3):
                        hop(p, h, r).wait_send()

        times = {(0, 0): 11.0, (0, 1): 18.0, (1, 0): 22.0, (1, 1): 25.5, (2, 0): 27.5, (2, 1): 29.0}
        out_events = [(self.lag, begin), (self.lag + 2.5, functools.partial(first, 0)), (self.lag + 3.0, functools.partial(first, 1))]
        for (p, h), t in times.items():
            out_events.append((self.lag + t, functools.partial(onward, p, h)))
        out_events.append((1e9, finish))
        return out_events


class Total:
    peers = "all"
    n_out = 1

    def __init__(self, blocks):
        self.blocks = blocks
        self.n_in = len(blocks)

    def inputs(self):
        return [(b, pl.BlockSpec(b.shape, lambda *_: (0, 0))) for b in self.blocks]

    def outputs(self):
        return [(jax.ShapeDtypeStruct((8, 128), F32), pl.BlockSpec((8, 128), lambda *_: (0, 0)))]

    def scratch(self):
        return [pltpu.VMEM((16, 8, 128), F32), pltpu.SemaphoreType.DMA((2, 16))]

    def run(self, here, ins, outs, scratch, last):
        (all_sums, sems), (out,) = scratch, outs

        def squares(ref):
            rows, cols = ref.shape

            def step(i, acc):
                g = ref[pl.ds(pl.multiple_of(i * 16, 16), 16), :].astype(F32)
                g = g * g
                return acc + sum(g[:, k * 128 : (k + 1) * 128] for k in range(cols // 128))

            s = lax.fori_loop(0, rows // 16, step, jnp.zeros((16, 128), F32))
            return s[:8] + s[8:]

        total = sum(squares(ref) for ref in (*ins, last))
        all_sums[here.me] = total
        copies = []
        for k in range(1, 16):
            to = lax.rem(here.me + k, 16)
            copies.append(send(all_sums.at[here.me], all_sums.at[here.me], sems, k, {"dp": to}))
        for c in copies:
            c.start()
        for c in copies:
            c.wait()
        total = all_sums[0]
        for k in range(1, 16):
            total = total + all_sums[k]
        out[...] = jnp.full((8, 128), jnp.sum(total), F32)


def stage(cid, name, steps, step_us, body, ins, outs, scratch=(), own_peers=(), comms=(), total=None, flops=0):
    comms = list(comms)
    everyone = comms + ([total] if total else [])
    args = [*ins] + [x for c in everyone for x in c.inputs()]
    results = [*outs] + [x for c in everyone for x in c.outputs()]
    temps = [*scratch] + [x for c in everyone for x in c.scratch()]
    peers = sorted({b for c in comms for b in c.peers} | set(own_peers))

    def kernel(*refs):
        here = Here()
        i, o = refs[: len(args)], refs[len(args) : len(args) + len(results)]
        s = refs[len(args) + len(results) :]
        at = pl.program_id(0)

        def barrier():
            sem = pltpu.get_barrier_semaphore()
            if total:
                for k in range(1, 16):
                    pl.semaphore_signal(sem, inc=1, device_id={"dp": lax.rem(here.me + k, 16)}, device_id_type=MESH)
                pl.semaphore_wait(sem, 15)
            else:
                for b in peers:
                    pl.semaphore_signal(sem, inc=1, device_id=here.peer(b), device_id_type=MESH)
                pl.semaphore_wait(sem, len(peers))

        events, ni, no, ns = [], len(ins), len(outs), len(scratch)
        for c in comms:
            ci, co, cs = i[ni : ni + c.n_in], o[no : no + c.n_out], s[ns : ns + len(c.scratch())]
            ni, no, ns = ni + c.n_in, no + c.n_out, ns + len(c.scratch())
            events += c.events(here, ci, co, cs)
        events.sort(key=lambda e: e[0])
        by_step = {}
        for t, fn in events:
            by_step.setdefault(min(steps, int(t / step_us)) if t < 1e9 else steps + 1, []).append(fn)

        def run(fns):
            for fn in fns:
                fn()

        @pl.when(at == 0)
        def _():
            if peers or total:
                barrier()
            run(by_step.get(0, []))

        for k in range(1, steps):
            if k in by_step:
                pl.when(at == k)(functools.partial(run, by_step[k]))
        if body:
            body(here, at, i[: len(ins)], o[: len(outs)], s[: len(scratch)])

        @pl.when(at == steps - 1)
        def _():
            run(by_step.get(steps, []) + by_step.get(steps + 1, []))
            if total:
                total.run(here, i[ni:], o[no:], s[ns:], o[no - 1])

    got = pl.pallas_call(
        kernel,
        grid=(steps,),
        in_specs=[spec for _, spec in args],
        out_specs=[spec for _, spec in results],
        out_shape=[shape for shape, _ in results],
        scratch_shapes=temps,
        compiler_params=pltpu.CompilerParams(
            collective_id=cid if (peers or total) else None, has_side_effects=bool(peers or total), vmem_limit_bytes=63 * 1024 * 1024
        ),
        name=name,
    )(*[a for a, _ in args])
    return got


def whole(array):
    return (array, pl.BlockSpec(array.shape, lambda *_: (0,) * array.ndim, pipeline_mode=pl.Buffered(1)))


def by_cols(array, width=TILE, last=None):
    lead = array.shape[:-1]
    return (array, pl.BlockSpec((*lead, width), lambda i: (0,) * len(lead) + (i if last is None else jnp.minimum(i, last),)))


def by_rows(array, height):
    return (array, pl.BlockSpec((height, array.shape[1]), lambda i: (i, 0)))


def new(shape, dtype, block, index):
    return (jax.ShapeDtypeStruct(shape, dtype), pl.BlockSpec(block, index))


def mm(a, b):
    return lax.dot_general(a, b, (((1,), (0,)), ((), ())), preferred_element_type=F32)


def mm_nt(a, b):
    return lax.dot_general(a, b, (((1,), (1,)), ((), ())), preferred_element_type=F32)


def chunks(total, size, fn):
    def step(i, _):
        fn(pl.ds(pl.multiple_of(i * size, size), size))
        return 0

    lax.fori_loop(0, total // size, step, 0)


def norm_of(wide):
    scale = lax.rsqrt(jnp.mean(wide * wide, -1, keepdims=True) + 1e-6)
    return (wide * scale).astype(BF16)


COL = lambda i: (0, i)
ROW = lambda i: (i, 0)


def norm_stage(cid, x, comms):
    def body(here, at, ins, outs, scratch):
        a = norm_of(ins[0][...].astype(F32))
        outs[0][...] = a
        outs[1][...] = a.T

    outs = [new((TOKENS, D), BF16, (256, D), ROW), new((D, TOKENS), BF16, (D, 256), COL)]
    return stage(cid, "norm", 8, 1.0, body, [by_rows(x, 256)], outs, comms=comms)


def gate_up_stage(cid, a, wg, wu, comms):
    def body(here, at, ins, outs, scratch):
        a, wg, wu = ins
        g_out, u_out, act_out, act_t = outs

        def part(rows):
            g = mm(a[rows, :], wg[...])
            u = mm(a[rows, :], wu[...])
            act = (g * jax.nn.sigmoid(g) * u).astype(BF16)
            g_out[rows, :] = g
            u_out[rows, :] = u
            act_out[rows, :] = act
            act_t[:, rows] = act.T

        chunks(TOKENS, 512, part)

    tile = (TOKENS, TILE)
    outs = [new((TOKENS, FF), t, tile, COL) for t in (F32, F32, BF16)] + [new((FF, TOKENS), BF16, (TILE, TOKENS), ROW)]
    return stage(cid, "gate_up", FF // TILE, 2.8, body, [whole(a), by_cols(wg), by_cols(wu)], outs, comms=comms)


def gate_stage(cid, a, wg, comms):
    def body(here, at, ins, outs, scratch):
        def part(rows):
            outs[0][rows, :] = mm(ins[0][rows, :], ins[1][...])

        chunks(TOKENS, 512, part)

    outs = [new((TOKENS, FF), F32, (TOKENS, TILE), COL)]
    return stage(cid, "gate", FF // TILE, 1.5, body, [whole(a), by_cols(wg)], outs, comms=comms)


def up_stage(cid, a, wu, g, comms):
    def body(here, at, ins, outs, scratch):
        a, wu, g_in = ins
        u_out, act_t = outs

        def part(rows):
            u = mm(a[rows, :], wu[...])
            g = g_in[rows, :]
            act = (g * jax.nn.sigmoid(g) * u).astype(BF16)
            u_out[rows, :] = u
            act_t[:, rows] = act.T

        chunks(TOKENS, 512, part)

    outs = [new((TOKENS, FF), F32, (TOKENS, TILE), COL), new((FF, TOKENS), BF16, (TILE, TOKENS), ROW)]
    return stage(cid, "up", FF // TILE, 1.5, body, [whole(a), by_cols(wu), by_cols(g)], outs, comms=comms)


def down_stage(cid, act, wd, x, comms):
    def body(here, at, ins, outs, scratch):
        act, wd, x = ins

        def part(rows):
            y = mm(act[rows, :], wd[...]).astype(BF16)
            h = x[rows, :] + y
            outs[0][rows, :] = h
            a = norm_of(h.astype(F32))
            outs[1][rows, :] = a
            outs[2][:, rows] = a.T

        chunks(512, 256, part)

    outs = [new((TOKENS, D), BF16, (512, D), ROW), new((TOKENS, D), BF16, (512, D), ROW), new((D, TOKENS), BF16, (D, 512), COL)]
    return stage(cid, "down", 4, 4.3, body, [by_rows(act, 512), whole(wd), by_rows(x, 512)], outs, comms=comms)


def dact_stage(cid, dy, wd, g, u, comms):
    def body(here, at, ins, outs, scratch):
        dy, wd, g_in, u_in = ins

        def part(rows):
            dact = mm_nt(dy[rows, :], wd[...]).astype(BF16).astype(F32)
            g, u = g_in[rows, :], u_in[rows, :]
            s = jax.nn.sigmoid(g)
            silu = g * s
            outs[0][rows, :] = (dact * u * (s + silu * (1.0 - s))).astype(BF16)
            outs[1][rows, :] = (dact * silu).astype(BF16)

        chunks(TOKENS, 512, part)

    outs = [new((TOKENS, FF), BF16, (TOKENS, TILE), COL)] * 2
    ins = [whole(dy), (wd, pl.BlockSpec((TILE, D), ROW)), by_cols(g), by_cols(u)]
    return stage(cid, "dact", FF // TILE, 1.5, body, ins, outs, comms=comms)


def dinput_stage(cid, dg, du, wg, wu, h, dy, comms):
    def body(here, at, ins, outs, scratch):
        dg, du, wg, wu, h, dy = ins

        def part(rows):
            da = mm_nt(dg[rows, :], wg[...]).astype(BF16) + mm_nt(du[rows, :], wu[...]).astype(BF16)
            da = da.astype(F32)
            wide = h[rows, :].astype(F32)
            scale = lax.rsqrt(jnp.mean(wide * wide, -1, keepdims=True) + 1e-6)
            along = jnp.mean(da * wide, -1, keepdims=True)
            dh = da * scale - wide * (scale * scale * scale * along)
            outs[0][rows, :] = dy[rows, :] + dh.astype(BF16)

        chunks(512, 256, part)

    outs = [new((TOKENS, D), BF16, (512, D), ROW)]
    ins = [by_rows(dg, 512), by_rows(du, 512), whole(wg), whole(wu), by_rows(h, 512), by_rows(dy, 512)]
    return stage(cid, "dinput", 4, 8.5, body, ins, outs, comms=comms)


def dw_stage(cid, left, right, comms):
    m, n = left.shape[0], right.shape[1]
    rows, tiles = m // 16, n // TILE
    group = 4 if rows == 80 else 2

    def body(here, at, ins, outs, scratch):
        left, right = ins
        acc, going, coming, sems = scratch
        core = here.bit[1]

        def swap(t):
            return send(going.at[t], coming.at[t], sems, t, here.peer(1))

        @pl.when(at < tiles)
        def _():
            slot = lax.rem(at, 2)

            def part(k, _):
                span = group * 2 * rows
                got = mm(left[pl.ds(pl.multiple_of(k * span, 16), span), :], right[...])
                acc[slot, pl.ds(k * group, group)] = got.reshape(group, 2, rows, TILE)
                return 0

            lax.fori_loop(0, 8 // group, part, 0)

            def put(k, _):
                going[at, k] = acc[slot, k, 1 - core].astype(BF16)
                return 0

            lax.fori_loop(0, 8, put, 0)
            swap(at).start()

        @pl.when(at > 0)
        def _():
            t = at - 1
            slot = lax.rem(t, 2)
            swap(t).wait()
            for a in range(2):
                for b in range(2):
                    for c in range(2):
                        k = a * 4 + b * 2 + c
                        outs[0][a, b, c] = acc[slot, k, core] + coming[t, k].astype(F32)

    back = lambda i: (0, 0, 0, 0, jnp.maximum(i - 1, 0))
    outs = [new((2, 2, 2, rows, n), F32, (2, 2, 2, rows, TILE), back)]
    scratch = [
        pltpu.VMEM((2, 8, 2, rows, TILE), F32),
        pltpu.VMEM((tiles, 8, rows, TILE), BF16),
        pltpu.VMEM((tiles, 8, rows, TILE), BF16),
        pltpu.SemaphoreType.DMA((2, tiles)),
    ]
    ins = [whole(left), by_cols(right, last=tiles - 1)]
    return stage(cid, "dw", tiles + 1, 17.5 / tiles, body, ins, outs, scratch, own_peers=(1,), comms=comms)


def adamw(w, m, v, g):
    m = 0.9 * m + 0.1 * g
    v = 0.95 * v + 0.05 * g * g
    step = m * lax.rsqrt(v + 1e-8) + 0.1 * w
    return (w - 0.02 * step).astype(jnp.bfloat16), m, v


def clipped(gradients, sum_of_squares, count):
    factor = jnp.minimum(1.0, 0.5 * lax.rsqrt(sum_of_squares / count + 1e-30))
    return [g * factor for g in gradients]


def solution(mesh):
    def step(x, dy, *arrays):
        weights, m, v = (arrays[i : i + 3] for i in (0, 3, 6))
        wg, wu, wd = weights
        x, dy = x[0], dy[0]
        up2 = lambda w: w.reshape(D, FF)
        down2 = lambda w: w.reshape(FF, D)

        a0, a0_t, wg0, wu0 = norm_stage(0, x, [Gather(wg, 0), Gather(wu, 0, 0.5)])
        g0, u0, act0, act0_t, wd0 = gate_up_stage(1, a0, up2(wg0), up2(wu0), [Gather(wd, 0)])
        h1, a1, a1_t, wg1 = down_stage(2, act0, down2(wd0), x, [Gather(wg, 1)])
        g1, wu1 = gate_stage(3, a1, up2(wg1), [Gather(wu, 1)])
        u1, act1_t, wd1 = up_stage(4, a1, up2(wu1), g1, [Gather(wd, 1)])
        (s_d1,) = dw_stage(5, act1_t, dy, [])
        dg1, du1, r_d1 = dact_stage(6, dy, down2(wd1), g1, u1, [Scatter(s_d1)])
        (s_g1,) = dw_stage(7, a1_t, dg1, [])
        s_u1, r_g1 = dw_stage(8, a1_t, du1, [Scatter(s_g1)])
        dh1, r_u1 = dinput_stage(9, dg1, du1, up2(wg1), up2(wu1), h1, dy, [Scatter(s_u1)])
        dg0, du0 = dact_stage(10, dh1, down2(wd0), g0, u0, [])
        (s_d0,) = dw_stage(11, act0_t, dh1, [])
        s_g0, r_d0 = dw_stage(12, a0_t, dg0, [Scatter(s_d0)])
        s_u0, r_g0 = dw_stage(13, a0_t, du0, [Scatter(s_g0)])
        r_u0, squares = stage(14, "last", 1, 1.0, None, [], [], comms=[Scatter(s_u0)], total=Total([r_d1, r_g1, r_u1, r_d0, r_g0]))

        gradients = [jnp.stack(pair).astype(F32) for pair in ((r_g0, r_g1), (r_u0, r_u1), (r_d0, r_d1))]
        gradients = clipped(gradients, squares[0, 0], 16 * sum(g.size for g in gradients))
        new_ = [adamw(w.astype(F32), m, v, g) for w, m, v, g in zip(weights, m, v, gradients, strict=True)]
        return tuple(one[which] for which in range(3) for one in new_)

    states, cut = P(("rep", "dp"), None, None), P(None, "dp", None)
    return jax.shard_map(
        step,
        mesh=mesh,
        in_specs=(states, states) + (cut,) * 9,
        out_specs=(P("rep", "dp", None),) * 9,
        check_vma=False,
    )
```

```python
import functools

import jax
import jax.numpy as jnp
from jax import lax
from jax.experimental import pallas as pl
from jax.experimental.pallas import tpu as pltpu
from jax.sharding import PartitionSpec as P

MESH = pl.DeviceIdType.MESH
F32, BF16 = jnp.float32, jnp.bfloat16
ANY = pl.BlockSpec(memory_space=pl.ANY)
BITS = (8, 4, 2, 1)
AXES = BITS[:3]
TURNS = ((8, 4, 2), (4, 2, 8), (2, 8, 4))
TOKENS, D, FF = 2048, 1280, 3072
NIL, SPAN = 0, 256
PAIR, THIRDS = range(2), range(3)


class Here:
    def __init__(self):
        me = lax.axis_index("dp")
        self.me = me
        self.bit = {b: lax.rem(lax.div(me, b), 2) for b in BITS}

    def peer(self, b):
        return {"dp": self.me + b * (1 - 2 * self.bit[b])}

    def at(self, how):
        out = []
        for b, h in how:
            out.append(self.bit[b] if h == "m" else 1 - self.bit[b] if h == "o" else slice(None))
        return tuple(out)


def send(src, dst, sems, i, device):
    return pltpu.make_async_remote_copy(
        src_ref=src, dst_ref=dst, send_sem=sems.at[NIL, i], recv_sem=sems.at[1, i], device_id=device, device_id_type=MESH
    )


def pieces(rows, cols):
    if cols == FF:
        wide = FF // 6
        return [[(slice(NIL, rows), slice((h * 3 + r) * wide, (h * 3 + r + 1) * wide)) for r in THIRDS] for h in PAIR]
    third, half = rows // 3, cols // 2
    return [[(slice(r * third, (r + 1) * third), slice(h * half, (h + 1) * half)) for r in THIRDS] for h in PAIR]


class Gather:
    copies = 19

    def __init__(self, here, own, full, parts, sems, base, turned=NIL, rest=False):
        self.rest = rest
        self.here, self.own, self.full, self.parts = here, own, full, parts
        self.sems, self.base = sems, base
        self.turns = [TURNS[(r + turned) % 3] for r in THIRDS]

    def view(self, how, r):
        return self.full.at[self.here.at([(b, how.get(b, "m")) for b in BITS]) + self.parts[r]]

    def hop(self, p, r):
        d = self.turns[r]
        dst = self.view({b: "f" for b in d[:p]}, r)
        src = self.own.at[self.parts[r]] if p == NIL else dst
        return send(src, dst, self.sems, self.base + p * 3 + r, self.here.peer(d[p]))

    def across(self, p, r):
        d = self.turns[r]
        ref = self.view({**{b: "f" for b in d[:p]}, d[p]: "o"}, r)
        return send(ref, ref, self.sems, self.base + 9 + p * 3 + r, self.here.peer(1))

    def place(self):
        return self.full.at[self.here.at([(b, "m") for b in BITS])]

    def own_across(self):
        return send(self.own, self.place(), self.sems, self.base + 18, self.here.peer(1))

    def keep(self):
        return pltpu.make_async_copy(self.own, self.place(), self.sems.at[2, self.base])

    def begin(self):
        for r in THIRDS:
            self.hop(NIL, r).start()
        if not self.rest:
            self.keep().start()
            self.own_across().start()

    def onward(self, p):
        if p == NIL and not self.rest:
            self.keep().wait()
        for r in THIRDS:
            self.hop(p, r).wait_recv()
            if p < 2:
                self.hop(p + 1, r).start()
            self.across(p, r).start()

    def arrived(self):
        for p in THIRDS:
            for r in THIRDS:
                self.across(p, r).wait_recv()
        if not self.rest:
            self.own_across().wait_recv()

    def finish(self):
        for p in THIRDS:
            for r in THIRDS:
                self.hop(p, r).wait_send()
                self.across(p, r).wait_send()
        if not self.rest:
            self.own_across().wait_send()


def cuts(widths, lead):
    out, at = [], NIL
    for w in widths:
        out.append((slice(None),) * lead + (slice(at, at + w),))
        at += w
    return out


class Scatter:
    peers = AXES
    n_out = 1

    def __init__(self, sums, number, lag=0.0, halves=(NIL, 1), ready=None, shape=None):
        self.array, self.number, self.halves = sums, number, halves
        self.rows, self.cols = shape or sums.shape[4:]
        self.lag, self.ready = lag, ready
        self.n_in = NIL if ready else 1

    def inputs(self):
        return [] if self.ready else [(self.array, ANY)]

    def outputs(self):
        spec = pl.BlockSpec((self.rows, self.width()), lambda *_: (NIL, NIL), pipeline_mode=pl.Buffered(1))
        return [(jax.ShapeDtypeStruct((self.rows, self.width()), BF16), spec)]

    def width(self):
        return self.cols * len(self.halves) // 2

    def scratch(self):
        r, c = pieces(self.rows, self.cols)[NIL][NIL]
        r, c = r.stop - r.start, c.stop - c.start
        legs = [pltpu.VMEM((3 * len(self.halves), *lead, r, c), BF16) for lead in ((2, 2), (2,), ())]
        return [pltpu.VMEM((2, 2, 2, self.rows, self.width()), F32), *legs, *legs, pltpu.SemaphoreType.DMA((2, 18)), pltpu.SemaphoreType.DMA]

    def events(self, here, ins, outs, scratch):
        (out,) = outs
        held, *legs, wire, local = scratch
        self.held = held
        going, coming = legs[:3], legs[3:]
        parts = pieces(self.rows, self.cols)
        if not self.ready:
            sums = ins[NIL]
        if len(self.halves) == 1:
            sums = sums.at[:, :, :, :, :, pl.ds(self.halves[NIL] * self.width(), self.width())]
        load = None if self.ready else pltpu.make_async_copy(sums.at[self.number], held, local)

        def place(order, picks):
            where = dict(zip(order, picks, strict=True))
            return tuple(where[b] for b in AXES)

        def hop(p, h, r):
            q = h * 3 + r
            return send(going[p].at[q], coming[p].at[q], wire, p * 6 + q, here.peer(TURNS[r][p]))

        count = len(self.halves)

        def begin():
            load.start()

        def first(h):
            if h == NIL and load:
                load.wait()
            for r in THIRDS:
                d, q = TURNS[r], h * 3 + r
                for i in PAIR:
                    for j in PAIR:
                        going[NIL][q, i, j] = held[place(d, (1 - here.bit[d[NIL]], i, j)) + parts[h][r]].astype(BF16)
                hop(NIL, h, r).start()

        def onward(p, h):
            for r in THIRDS:
                d, q = TURNS[r], h * 3 + r
                mine = [here.bit[b] for b in d]
                hop(p, h, r).wait_recv()
                if p == NIL:
                    for j in PAIR:
                        at = place(d, (mine[NIL], 1 - mine[1], j)) + parts[h][r]
                        going[1][q, j] = (held[at] + coming[NIL][q, 1 - mine[1], j].astype(F32)).astype(BF16)
                    hop(1, h, r).start()
                    for j in PAIR:
                        at = place(d, (mine[NIL], mine[1], j)) + parts[h][r]
                        held[at] = held[at] + coming[NIL][q, mine[1], j].astype(F32)
                elif p == 1:
                    at = place(d, (mine[NIL], mine[1], 1 - mine[2])) + parts[h][r]
                    going[2][q] = (held[at] + coming[1][q, 1 - mine[2]].astype(F32)).astype(BF16)
                    hop(2, h, r).start()
                    at = place(d, mine) + parts[h][r]
                    held[at] = held[at] + coming[1][q, mine[2]].astype(F32)
                else:
                    at = place(d, mine) + parts[h][r]
                    out[parts[h][r]] = (held[at] + coming[2][q].astype(F32)).astype(BF16)

        def finish():
            for p in THIRDS:
                for h in range(count):
                    for r in THIRDS:
                        hop(p, h, r).wait_send()

        times = {(NIL, NIL): 12.0, (NIL, 1): 19.0, (1, NIL): 23.0, (1, 1): 26.5, (2, NIL): 28.5, (2, 1): 30.0}
        if count == 1:
            times = {(NIL, NIL): 12.0, (1, NIL): 17.5, (2, NIL): 21.0}
        if self.ready:
            out_events = [(step, functools.partial(first, h)) for h, step in enumerate(self.ready)]
        else:
            out_events = [(self.lag, begin)] + [(self.lag + HOP_US + h / 2, functools.partial(first, h)) for h in range(count)]
        for (p, h), t in times.items():
            out_events.append((self.lag + t, functools.partial(onward, p, h)))
        out_events.append((1e9, finish))
        return out_events


class Total:
    peers = "all"
    n_out = 1

    def __init__(self, blocks):
        self.blocks = blocks
        self.n_in = len(blocks)

    def inputs(self):
        return [whole(b) for b in self.blocks]

    def outputs(self):
        return [(jax.ShapeDtypeStruct((8, 128), F32), pl.BlockSpec((8, 128), lambda *_: (NIL, NIL)))]

    def scratch(self):
        return [pltpu.VMEM((16, 8, 128), F32), pltpu.SemaphoreType.DMA((2, 16))]

    def run(self, here, ins, outs, scratch, lasts):
        (all_sums, sems), (out,) = scratch, outs

        def squares(ref):
            rows, cols = ref.shape

            def step(i, acc):
                g = ref[pl.ds(pl.multiple_of(i * 16, 16), 16), :].astype(F32)
                g = g * g
                return acc + sum(g[:, k * 128 : (k + 1) * 128] for k in range(cols // 128))

            s = lax.fori_loop(NIL, rows // 16, step, jnp.zeros((16, 128), F32))
            return s[:8] + s[8:]

        total = sum(squares(ref) for ref in (*ins, *lasts))
        all_sums[here.me] = total
        copies = []
        for k in range(1, 16):
            to = lax.rem(here.me + k, 16)
            copies.append(send(all_sums.at[here.me], all_sums.at[here.me], sems, k, {"dp": to}))
        for c in copies:
            c.start()
        for c in copies:
            c.wait()
        total = all_sums[NIL]
        for k in range(1, 16):
            total = total + all_sums[k]
        out[...] = jnp.full((8, 128), jnp.sum(total), F32)


def stage(cid, name, steps, step_us, body, ins, outs, scratch=(), own_peers=(), comms=(), total=None, flops=NIL):
    comms = list(comms)
    everyone = comms + ([total] if total else [])
    args = [*ins] + [x for c in everyone for x in c.inputs()]
    results = [*outs] + [x for c in everyone for x in c.outputs()]
    temps = [*scratch] + [x for c in everyone for x in c.scratch()]
    peers = sorted({b for c in comms for b in c.peers} | set(own_peers))

    def kernel(*refs):
        here = Here()
        i, o = refs[: len(args)], refs[len(args) : len(args) + len(results)]
        s = refs[len(args) + len(results) :]
        at = pl.program_id(NIL)

        def barrier():
            sem = pltpu.get_barrier_semaphore()
            if total:
                for k in range(1, 16):
                    pl.semaphore_signal(sem, inc=1, device_id={"dp": lax.rem(here.me + k, 16)}, device_id_type=MESH)
                pl.semaphore_wait(sem, 15)
            else:
                for b in peers:
                    pl.semaphore_signal(sem, inc=1, device_id=here.peer(b), device_id_type=MESH)
                pl.semaphore_wait(sem, len(peers))

        events, ni, no, ns = [], len(ins), len(outs), len(scratch)
        for c in comms:
            ci, co, cs = i[ni : ni + c.n_in], o[no : no + c.n_out], s[ns : ns + len(c.scratch())]
            ni, no, ns = ni + c.n_in, no + c.n_out, ns + len(c.scratch())
            events += c.events(here, ci, co, cs)
        events.sort(key=lambda e: e[NIL] * step_us if isinstance(e[NIL], int) else e[NIL])
        by_step = {}
        for t, fn in events:
            k = t if isinstance(t, int) else int(t / step_us + 0.8)
            by_step.setdefault(min(steps, k) if t < 1e9 else steps + 1, []).append(fn)

        def run(fns):
            for fn in fns:
                fn()

        @pl.when(at == NIL)
        def _():
            if peers or total:
                barrier()
            run(by_step.get(NIL, []))

        for k in range(1, steps):
            if k in by_step:
                pl.when(at == k)(functools.partial(run, by_step[k]))
        if body:
            body(here, at, i[: len(ins)], o[: len(outs)], s[: len(scratch)])

        @pl.when(at == steps - 1)
        def _():
            run(by_step.get(steps, []) + by_step.get(steps + 1, []))
            if total:
                total.run(here, i[ni:], o[no:], s[ns:], o[len(outs) : no])

    got = pl.pallas_call(
        kernel,
        grid=(steps,),
        in_specs=[spec for _, spec in args],
        out_specs=[spec for _, spec in results],
        out_shape=[shape for shape, _ in results],
        scratch_shapes=temps,
        compiler_params=pltpu.CompilerParams(
            collective_id=cid if (peers or total) else None, has_side_effects=bool(peers or total), vmem_limit_bytes=63 * 1024 * 1024
        ),
        name=name,
    )(*[a for a, _ in args])
    return got


def whole(array):
    return (array, pl.BlockSpec(array.shape, lambda *_: (NIL,) * array.ndim, pipeline_mode=pl.Buffered(1)))


def by_rows(array, height):
    return (array, pl.BlockSpec((height, array.shape[1]), lambda i: (i, NIL)))


def new(shape, dtype, block, index):
    return (jax.ShapeDtypeStruct(shape, dtype), pl.BlockSpec(block, index))


def mm(a, b):
    return lax.dot_general(a, b, (((1,), (NIL,)), ((), ())), preferred_element_type=F32)


def mm_nt(a, b):
    return lax.dot_general(a, b, (((1,), (1,)), ((), ())), preferred_element_type=F32)


def norm_of(wide):
    scale = lax.rsqrt(jnp.mean(wide * wide, -1, keepdims=True) + 1e-6)
    return (wide * scale).astype(BF16)


COL = lambda s: (NIL, s)
ROW = lambda i: (i, NIL)


def sigmoid(g):
    return 0.5 * jnp.tanh(0.5 * g) + 0.5


def by_core(blocks, out, cols):
    rows = out.shape[2]
    for k in range(out.shape[1]):
        for c in PAIR:
            at = (2 * k + c) * rows
            out[c, k, :, cols] = blocks[at : at + rows, :]


WIDE = SPAN
UNITS = FF // WIDE
KINDS = 2, D // 16
CHUNK = FF // 3
WIRE_GU, WIRE_D = 16.8, 8.4
HOP_US, EARLY_US = 2.5, 6.0
CUT_GU, CUT_D = (384, 384, SPAN), (512, 384, 384)
PLACES = (2, 2, 2, 2)


def all_rows(fn):
    count = TOKENS // SPAN // 2

    def turn(j, _):
        for i in range(count):
            fn(pl.ds(pl.multiple_of((j * count + i) * SPAN, SPAN), SPAN))
        return NIL

    lax.fori_loop(NIL, 2, turn, NIL)


def tile_of(gu, c, which, q):
    return gu[c, :, :, :, :, which, :, pl.ds(pl.multiple_of(q * WIDE, WIDE), WIDE)].reshape(D, WIDE)


def by_third(block, out, c):
    out[...] = jnp.concatenate([block[:, n * 192 + c * 64 : n * 192 + c * 64 + 64] for n in range(16)], axis=1)


def barrier_of(here, peers):
    sem = pltpu.get_barrier_semaphore()
    for b in peers:
        pl.semaphore_signal(sem, inc=1, device_id=here.peer(b), device_id_type=MESH)
    pl.semaphore_wait(sem, len(peers))


def schedule(at, steps, table):
    by_step = {}
    for k, fn in table:
        by_step.setdefault(k, []).append(fn)
    for k, fns in by_step.items():

        @pl.when(at == k)
        def _(fns=fns):
            for fn in fns:
                fn()


def wire_order(units):
    legs = [("b", NIL)]
    for n in range(len(units)):
        legs += [("b", n + 1), (NIL, n + 1) if n else (NIL, NIL)] if n else [("b", 1), (NIL, NIL), ("b", 2), (NIL, 1)]
        legs += [(1, n)]
    order, seen = [], set()
    for leg in legs + [(NIL, n) for n in range(len(units))]:
        if leg not in seen and leg[1] < len(units):
            seen.add(leg)
            order.append(leg)
    wire, done, out, last = 0.0, {}, [], 0.0
    for kind, n in order:
        length, unit = units[n]
        if kind == "b":
            out.append((last, unit.begin, unit))
            wire = max(wire, last) + length / 7
            done[NIL, n] = wire
        else:
            last = max(last, done[kind, n] + HOP_US)
            out.append((last, functools.partial(unit.onward, kind), unit))
            wire = max(wire, last) + length * (2, 4)[kind] / 7
            done[kind + 1, n] = wire
    for n, (_, unit) in enumerate(units):
        unit.ready = done[2, n] + 4.0
        out.append((done[2, n] + HOP_US, functools.partial(unit.onward, 2), unit))
    return sorted(out, key=lambda e: e[NIL])


def placed(events, lengths, due):
    starts, now = [], 0.0
    for i, length in enumerate(lengths):
        now = max([now] + [unit.ready for step, unit in due if step == i])
        starts.append(now)
        now += length
    out = []
    for t, fn, unit in events:
        k = next((i for i, u in enumerate(starts) if u >= t - EARLY_US), len(starts))
        out.append((min([k] + [step for step, one in due if one is unit]), fn))
    return out


def call(cid, name, kernel, steps, ins, outs, scratch):
    return pl.pallas_call(
        kernel,
        grid=(steps,),
        in_specs=[spec for _, spec in ins],
        out_specs=[spec for _, spec in outs],
        out_shape=[shape for shape, _ in outs],
        scratch_shapes=scratch,
        compiler_params=pltpu.CompilerParams(collective_id=cid, has_side_effects=True, vmem_limit_bytes=67043328),
        name=name,
    )(*[a for a, _ in ins])


def blocks_of(array, *index):
    lead = len(index)
    block = (1,) * lead + array.shape[lead:]
    rest = (NIL,) * (array.ndim - lead)
    return (array, pl.BlockSpec(block, lambda s: index + rest, pipeline_mode=pl.Buffered(1)))


N1 = 8
G1 = N1 + UNITS
D1 = G1 + 4
E1 = D1 + 8


def first_stage(cid, x, wg, wu, wd):
    def kernel(x, wg, wu, wg1, wu1, wd_own, wd1_own, a_t, g_out, u_out, act_t, wd_full, h_out, a1_out, a1_t, gu1_full, wd1_full, *scratch):
        a, gu_all, wd_all, act, gu_own, gu1_own, sems, local = scratch
        wd_own, wd1_own = wd_own.at[NIL], wd1_own.at[NIL]
        here, at = Here(), pl.program_id(NIL)

        @pl.when(at == NIL)
        def _():
            for k, own in enumerate((wg, wu)):
                block = own[NIL]
                for c in THIRDS:
                    by_third(block, gu_own.at[c, k], c)
            for k, own in enumerate((wg1, wu1)):
                by_third(own[NIL], gu1_own.at[k], NIL)

        n = Gather.copies
        units = [Gather(here, gu_own.at[c], gu_all.at[c], cuts(CUT_GU, 2), sems, c * n, c) for c in THIRDS]
        halves = pieces(D3, D)
        units += [Gather(here, wd_own, wd_all, halves[h], sems, (3 + h) * n, rest=h == 1) for h in PAIR]
        units += [Gather(here, gu1_own, gu1_full, cuts(CUT_GU, 2), sems, 5 * n)]
        units += [Gather(here, wd1_own, wd1_full, cuts(CUT_D, 1), sems, 6 * n, 2)]

        timed = [(WIRE_D if i == 6 else WIRE_D * 1.5 if i in (3, 4) else WIRE_GU, unit) for i, unit in enumerate(units)]
        lengths = [1.0] * N1 + [3.6] * UNITS + [5.0] * (D1 - G1) + [1.0] * N1
        due = [(N1, units[NIL]), (N1 + 4, units[1]), (N1 + 8, units[2]), (G1, units[3]), (G1 + 2, units[4])]
        events = placed(wire_order(timed), lengths, due)
        waits = [(k, unit.arrived) for k, unit in due]
        spill = pltpu.make_async_copy(wd_all, wd_full, local)

        schedule(at, E1, [(NIL, functools.partial(barrier_of, here, BITS))])
        schedule(at, E1, [e for e in events if e[NIL] < E1])
        schedule(at, E1, waits)

        @pl.when(at < N1)
        def _():
            normed = norm_of(x[...].astype(F32))
            a[pl.ds(pl.multiple_of(at * SPAN, SPAN), SPAN), :] = normed
            by_core(normed.T, a_t, slice(None))

        @pl.when((at >= N1) & (at < G1))
        def _():
            t = at - N1
            c, q = lax.div(t, 4), lax.rem(t, 4)
            def part(rows):
                g = mm(a[rows, :], tile_of(gu_all, c, NIL, q))
                u = mm(a[rows, :], tile_of(gu_all, c, 1, q))
                v = (g * sigmoid(g) * u).astype(BF16)
                g_out[rows, :] = g
                u_out[rows, :] = u
                act[t, rows, :] = v
                by_core(v.T, act_t, rows)

            all_rows(part)

        @pl.when((at >= G1) & (at < D1))
        def _():
            t = at - G1
            cols = pl.ds(pl.multiple_of(lax.div(t, 2) * 640, 128), 640)
            for i in range(4):
                rows = pl.ds(pl.multiple_of(lax.rem(t, 2) * 1024 + i * SPAN, SPAN), SPAN)
                y = jnp.zeros((SPAN, 640), F32)
                for c in THIRDS:
                    left = jnp.concatenate([act[c * 4 + q, rows, :] for q in range(4)], axis=1)
                    y = y + mm(left, wd_all[:, :, :, :, c * 64 : (c + 1) * 64, cols].reshape(CHUNK, 640))
                a[rows, cols] = y.astype(BF16)

        @pl.when(at == D1)
        def _():
            spill.start()

        @pl.when(at >= D1)
        def _():
            h = x[...] + a[pl.ds(pl.multiple_of((at - D1) * SPAN, SPAN), SPAN), :]
            h_out[...] = h
            normed = norm_of(h.astype(F32))
            a1_out[...] = normed
            by_core(normed.T, a1_t, slice(None))

        @pl.when(at == E1 - 1)
        def _():
            for k, fn in events:
                if k >= E1:
                    fn()
            for unit in units[5:]:
                unit.arrived()
            for unit in units:
                unit.finish()
            spill.wait()

    D3 = FF // 16
    tile = lambda s: jnp.clip(s - N1, NIL, UNITS - 1)
    early = lambda s: jnp.minimum(s, N1 - 1)
    late = lambda s: jnp.maximum(s - D1, NIL)
    strip = (2, 8, D // 16, TOKENS)
    outs = [
        new(strip, BF16, (*strip[:3], SPAN), lambda s: (NIL, NIL, NIL, early(s))),
        new((TOKENS, FF), F32, (TOKENS, WIDE), lambda s: (NIL, tile(s))),
        new((TOKENS, FF), F32, (TOKENS, WIDE), lambda s: (NIL, tile(s))),
        new((2, 8, D3, TOKENS), BF16, (2, 2, 64, TOKENS), lambda s: (NIL, lax.rem(tile(s), 4), lax.div(tile(s), 4), NIL)),
        (jax.ShapeDtypeStruct((*PLACES, D3, D), BF16), ANY),
        new((TOKENS, D), BF16, (SPAN, D), lambda s: (late(s), NIL)),
        new((TOKENS, D), BF16, (SPAN, D), lambda s: (late(s), NIL)),
        new(strip, BF16, (*strip[:3], SPAN), lambda s: (NIL, NIL, NIL, late(s))),
        (jax.ShapeDtypeStruct((*PLACES, *KINDS, CHUNK), BF16), ANY),
        (jax.ShapeDtypeStruct((*PLACES, 64, D), BF16), ANY),
    ]
    ins = [(x, pl.BlockSpec((SPAN, D), lambda s: (jnp.where(s < D1, early(s), late(s)), NIL)))]
    ins += [blocks_of(wg, NIL), blocks_of(wu, NIL), blocks_of(wg, 1), blocks_of(wu, 1), blocks_of(wd, NIL)]
    ins += [(wd, pl.BlockSpec((1, 64, D), lambda s: (1, NIL, NIL), pipeline_mode=pl.Buffered(1)))]
    scratch = [
        pltpu.VMEM((TOKENS, D), BF16),
        pltpu.VMEM((3, *PLACES, *KINDS, CHUNK), BF16),
        pltpu.VMEM((*PLACES, D3, D), BF16),
        pltpu.VMEM((UNITS, TOKENS, WIDE), BF16),
        pltpu.VMEM((3, *KINDS, CHUNK), BF16),
        pltpu.VMEM((*KINDS, CHUNK), BF16),
        pltpu.SemaphoreType.DMA((3, 7 * Gather.copies)),
        pltpu.SemaphoreType.DMA,
    ]
    return call(cid, "first", kernel, E1, ins, outs, scratch)


def second_stage(cid, a, dy, wg, wu, wd, gu_first, wd_first):
    def kernel(a_in, dy_in, wg, wu, wd_own, gu_first, wd_first, dgu, act_t, gu_rest, *scratch):
        gu_all, wd_all, gu_own, a, dy, sems, local = scratch
        wd_own = wd_own.at[NIL]
        here, at = Here(), pl.program_id(NIL)

        @pl.when(at == NIL)
        def _():
            for k, own in enumerate((wg, wu)):
                block = own[NIL]
                for c in (1, 2):
                    by_third(block, gu_own.at[c - 1, k], c)

        n = Gather.copies
        units = []
        for c in (1, 2):
            units.append(Gather(here, gu_own.at[c - 1], gu_all.at[c], cuts(CUT_GU, 2), sems, len(units) * n, c))
            units.append(Gather(here, wd_own.at[pl.ds(c * 64, 64)], wd_all.at[c], cuts(CUT_D, 1), sems, len(units) * n, c + 2))
        timed = list(zip((WIRE_GU, WIRE_D) * 2, units, strict=True))
        due = [(4, units[NIL]), (4, units[1]), (8, units[2]), (8, units[3])]
        events = placed(wire_order(timed), [5.6] * UNITS, due)
        moves = ((a_in, a), (gu_first, gu_all.at[NIL]), (dy_in, dy), (wd_first, wd_all.at[NIL]))
        loads = [pltpu.make_async_copy(src, dst, local.at[i]) for i, (src, dst) in enumerate(moves)]
        spills = [pltpu.make_async_copy(gu_all.at[c], gu_rest.at[c - 1], local.at[3 + c]) for c in (1, 2)]
        table = [(NIL, load.start) for load in loads] + [(NIL, functools.partial(barrier_of, here, BITS))]
        table += [e for e in events if e[NIL] < UNITS]
        table += [(NIL, load.wait) for load in loads]
        table += [(k, unit.arrived) for k, unit in due] + [(4, spills[NIL].start), (8, spills[1].start)]
        schedule(at, UNITS, table)

        c, q = lax.div(at, 4), lax.rem(at, 4)
        qx, qy = lax.div(q, 2), lax.rem(q, 2)
        def part(rows):
            g = mm(a[rows, :], tile_of(gu_all, c, NIL, q))
            u = mm(a[rows, :], tile_of(gu_all, c, 1, q))
            dact = mm_nt(dy[rows, :], wd_all[c, qx, qy].reshape(WIDE, D)).astype(BF16).astype(F32)
            s = sigmoid(g)
            silu = g * s
            by_core((silu * u).astype(BF16).T, act_t, rows)
            dgu[NIL, rows, :] = (dact * u * (s + silu * (1.0 - s))).astype(BF16)
            dgu[1, rows, :] = (dact * silu).astype(BF16)

        all_rows(part)

        @pl.when(at == UNITS - 1)
        def _():
            for unit in units:
                unit.finish()
            for s in spills:
                s.wait()

    outs = [
        new((2, TOKENS, FF), BF16, (2, TOKENS, WIDE), lambda s: (NIL, NIL, s)),
        new((2, 8, FF // 16, TOKENS), BF16, (2, 2, 64, TOKENS), lambda s: (NIL, lax.rem(s, 4), lax.div(s, 4), NIL)),
        (jax.ShapeDtypeStruct((2, *PLACES, *KINDS, CHUNK), BF16), ANY),
    ]
    ins = [(a, ANY), (dy, ANY), blocks_of(wg, 1), blocks_of(wu, 1), blocks_of(wd, 1), (gu_first, ANY), (wd_first, ANY)]
    scratch = [
        pltpu.VMEM((3, *PLACES, *KINDS, CHUNK), BF16),
        pltpu.VMEM((3, *PLACES, 64, D), BF16),
        pltpu.VMEM((2, *KINDS, CHUNK), BF16),
        *[pltpu.VMEM((TOKENS, D), BF16)] * 2,
        pltpu.SemaphoreType.DMA((3, 4 * Gather.copies)),
        pltpu.SemaphoreType.DMA((6,)),
    ]
    return call(cid, "second", kernel, UNITS, ins, outs, scratch)


def dact_stage(cid, dy, wd, g, u, comms):
    def body(here, at, ins, outs, scratch):
        dy, wd, g_in, u_in = ins
        def part(rows):
            dact = mm_nt(dy[rows, :], wd[...].reshape(WIDE, D)).astype(BF16).astype(F32)
            g, u = g_in[rows, :], u_in[rows, :]
            s = sigmoid(g)
            silu = g * s
            outs[NIL][NIL, rows, :] = (dact * u * (s + silu * (1.0 - s))).astype(BF16)
            outs[NIL][1, rows, :] = (dact * silu).astype(BF16)

        all_rows(part)

    outs = [new((2, TOKENS, FF), BF16, (2, TOKENS, WIDE), lambda s: (NIL, NIL, s))]
    tile = pl.BlockSpec((TOKENS, WIDE), COL)
    ins = [whole(dy), (wd, pl.BlockSpec((4, 64, D), lambda s: (lax.rem(s, 4), lax.div(s, 4), NIL))), (g, tile), (u, tile)]
    return stage(cid, "dact", UNITS, 2.5, body, ins, outs, comms=comms)


def dinput_stage(cid, dgu, gu_first, gu_rest, h, dy, comms):
    def body(here, at, ins, outs, scratch):
        dgu, gu_first, gu_rest, h, dy = ins
        back = []
        for k in PAIR:
            total = mm_nt(dgu[k, :, :CHUNK], gu_first[:, :, :, :, k].reshape(D, CHUNK))
            for c in range(1, 3):
                total += mm_nt(dgu[k, :, c * CHUNK : (c + 1) * CHUNK], gu_rest[c - 1, :, :, :, :, k].reshape(D, CHUNK))
            back.append(total.astype(BF16))
        da = (back[NIL] + back[1]).astype(F32)
        wide = h[...].astype(F32)
        scale = lax.rsqrt(jnp.mean(wide * wide, -1, keepdims=True) + 1e-6)
        along = jnp.mean(da * wide, -1, keepdims=True)
        dh = da * scale - wide * (scale * scale * scale * along)
        outs[NIL][...] = dy[...] + dh.astype(BF16)

    outs = [new((TOKENS, D), BF16, (SPAN, D), ROW)]
    ins = [(dgu, pl.BlockSpec((2, SPAN, FF), lambda i: (NIL, i, NIL))), whole(gu_first), whole(gu_rest), by_rows(h, SPAN), by_rows(dy, SPAN)]
    return stage(cid, "dinput", 8, 5.2, body, ins, outs, comms=comms)


def dw_stage(cid, left, right, comms, into=(), total=None):
    rows, (count, _, n) = left.shape[2], right.shape
    width = 512 if n == FF else SPAN
    per = n // width
    turn = 2 * per

    def body(here, at, ins, outs, scratch):
        left_in, right = ins
        left, going, coming, sems, local = scratch
        core = here.bit[1]
        step = 4 if rows == 80 else 2
        matrix, place = lax.div(at, turn), lax.rem(at, turn)

        def load(c):
            return pltpu.make_async_copy(left_in.at[c], left.at[c], local.at[c])

        @pl.when(at == NIL)
        def _():
            load(1 - core).start()
            load(core).start()
            load(1 - core).wait()

        @pl.when(at == per)
        def _():
            load(core).wait()

        def swap(t):
            one = matrix * per + t
            return send(going.at[t], coming.at[one], sems, one, here.peer(1))

        @pl.when(place < per)
        def _():
            for k in range(NIL, 8, step):
                a = left[1 - core, k : k + step].reshape(step * rows, TOKENS)
                going[place, k : k + step] = mm(a, right[NIL]).astype(BF16).reshape(step, rows, width)
            swap(place).start()

        def own(put):
            t = place - per
            swap(t).wait()
            for k in range(NIL, 8, step):
                a = left[core, k : k + step].reshape(step * rows, TOKENS)
                got = mm(a, right[NIL]).reshape(step, rows, width)
                for i in range(step):
                    where = (k + i) // 4, (k + i) // 2 % 2, (k + i) % 2
                    put(where, t, got[i] + coming[matrix * per + t, k + i].astype(F32))

        def put_out(where, t, value):
            outs[NIL][(NIL, *where)] = value

        if into:
            for m, scatter in enumerate(into):

                def put_held(where, t, value, held=scatter.held):
                    held[(*where, slice(None), pl.ds(pl.multiple_of(t * width, width), width))] = value

                pl.when((place >= per) & (matrix == m))(functools.partial(own, put_held))
        else:
            pl.when(place >= per)(functools.partial(own, put_out))

    def source(s):
        return (lax.div(s, turn), NIL, lax.rem(lax.rem(s, turn), per))

    def back(s):
        return (lax.div(s, turn), NIL, NIL, NIL, NIL, jnp.maximum(lax.rem(s, turn) - per, NIL))

    outs = [] if into else [new((count, 2, 2, 2, rows, n), F32, (1, 2, 2, 2, rows, width), back)]
    scratch = [pltpu.VMEM(left.shape, BF16), pltpu.VMEM((per, 8, rows, width), BF16), pltpu.VMEM((count * per, 8, rows, width), BF16)]
    scratch += [pltpu.SemaphoreType.DMA((2, count * per)), pltpu.SemaphoreType.DMA((2,))]
    ins = [(left, ANY), (right, pl.BlockSpec((1, TOKENS, width), source))]
    steps = count * turn
    return stage(cid, "dw", steps, count * 21.0 / steps, body, ins, outs, scratch, own_peers=(1,), comms=[*comms, *into], total=total)


def update_stage(weights, moments, seconds, sums, squares):
    steps = 5
    flat = [piece for pair in sums for layer in pair for piece in layer]
    count = 16 * sum(w.size for w in weights)

    def kernel(*refs):
        squares, ws, ms, vs = refs[NIL], refs[1:4], refs[4:7], refs[7:10]
        pieces_in, outs = list(refs[10 : 10 + len(flat)]), refs[10 + len(flat) :]
        factor = jnp.minimum(1.0, 0.5 * lax.rsqrt(squares[...] / count + 1e-30))[:1, :1]
        for i in THIRDS:
            for n in PAIR:
                taken = [pieces_in.pop(NIL) for _ in sums[i][n]]
                g = jnp.concatenate([r[...].astype(F32) for r in taken], axis=1) if len(taken) > 1 else taken[NIL][...].astype(F32)
                if i < 2:
                    at = [c * CHUNK + k * 64 for k in range(16) for c in THIRDS]
                    g = jnp.concatenate([g[:, u : u + 64] for u in at], axis=1)
                g = g * factor
                m = 0.9 * ms[i][n] + 0.1 * g
                v = 0.95 * vs[i][n] + 0.05 * g * g
                w = ws[i][n].astype(F32)
                outs[i][n] = (w - 0.02 * (m * lax.rsqrt(v + 1e-8) + 0.1 * w)).astype(BF16)
                outs[3 + i][n] = m
                outs[6 + i][n] = v

    def spec(array):
        lead = array.ndim - 2
        rows, cols = array.shape[lead:]
        height = 16 if rows == D // 16 else 48
        last = rows // height - 1
        return pl.BlockSpec((2,) * lead + (height, cols), lambda s: (NIL,) * lead + (jnp.minimum(s, last), NIL))

    args = [*weights, *moments, *seconds, *flat]
    like = [*weights, *moments, *seconds]
    return pl.pallas_call(
        kernel,
        grid=(steps,),
        in_specs=[pl.BlockSpec((8, 128), lambda s: (NIL, NIL))] + [spec(a) for a in args],
        out_specs=[spec(a) for a in like],
        out_shape=[jax.ShapeDtypeStruct(a.shape, a.dtype) for a in like],
        compiler_params=pltpu.CompilerParams(vmem_limit_bytes=60 * 1024 * 1024),
        name="update",
    )(squares, *args)


def solution(mesh):
    def step(x, dy, *arrays):
        weights, m, v = (arrays[i : i + 3] for i in (NIL, 3, 6))
        wg, wu, wd = weights
        x, dy = x[NIL], dy[NIL]
        a0_t, g0, u0, act0_t, wd0, h1, a1, a1_t, gu1_first, wd1_first = first_stage(NIL, x, wg, wu, wd)
        dgu1, act1_t, gu1_rest = second_stage(1, a1, dy, wg, wu, wd, gu1_first, wd1_first)
        (s_d1,) = dw_stage(9, act1_t, dy[None], [])
        s_1, r_d1 = dw_stage(2, a1_t, dgu1, [Scatter(s_d1, NIL)])
        dh1, r_g1 = dinput_stage(3, dgu1, gu1_first, gu1_rest, h1, dy, [Scatter(s_1, NIL)])
        s_d0, r_u1a = dw_stage(4, act0_t, dh1[None], [Scatter(s_1, 1, halves=(NIL,))])
        early = [Scatter(s_1, 1, halves=(1,)), Scatter(s_d0, NIL, 11.0, halves=(NIL,))]
        dgu0, r_u1b, r_d0a = dact_stage(5, dh1, wd0.reshape(16, FF // 16, D), g0, u0, early)
        block = (D // 16, FF)
        late = [Scatter(None, NIL, 14.0, ready=(9, 12), shape=block), Scatter(None, NIL, 40.0, ready=(21, 24), shape=block)]
        total = Total([r_d1, r_g1, r_u1a, r_u1b, r_d0a])
        r_d0b, r_g0, r_u0, squares = dw_stage(6, a0_t, dgu0, [Scatter(s_d0, NIL, halves=(1,))], late, total)
        sums = (((r_g0,), (r_g1,)), ((r_u0,), (r_u1a, r_u1b)), ((r_d0a, r_d0b), (r_d1,)))
        return tuple(update_stage(weights, m, v, sums, squares))

    states, cut = P(("rep", "dp"), None, None), P(None, "dp", None)
    return jax.shard_map(
        step,
        mesh=mesh,
        in_specs=(states, states) + (cut,) * 9,
        out_specs=(P("rep", "dp", None),) * 9,
        check_vma=False,
    )
```

```python
import functools

import jax
import jax.numpy as jnp
from jax import lax
from jax.experimental import pallas as pl
from jax.experimental.pallas import tpu as pltpu
from jax.sharding import PartitionSpec as P

MESH = pl.DeviceIdType.MESH
F32, BF16 = jnp.float32, jnp.bfloat16
ANY = pl.BlockSpec(memory_space=pl.ANY)
BITS = (8, 4, 2, 1)
AXES = BITS[:3]
TURNS = ((8, 4, 2), (4, 2, 8), (2, 8, 4))
TOKENS, D, FF = 2048, 1280, 3072
NIL, SPAN = 0, 256
PAIR, THIRDS = range(2), range(3)


class Here:
    def __init__(self):
        me = lax.axis_index("dp")
        self.me = me
        self.bit = {b: lax.rem(lax.div(me, b), 2) for b in BITS}

    def peer(self, b):
        return {"dp": self.me + b * (1 - 2 * self.bit[b])}

    def at(self, how):
        out = []
        for b, h in how:
            out.append(self.bit[b] if h == "m" else 1 - self.bit[b] if h == "o" else slice(None))
        return tuple(out)


def send(src, dst, sems, i, device):
    return pltpu.make_async_remote_copy(
        src_ref=src, dst_ref=dst, send_sem=sems.at[NIL, i], recv_sem=sems.at[1, i], device_id=device, device_id_type=MESH
    )


def pieces(rows, cols):
    if cols == FF:
        wide = FF // 6
        return [[(slice(NIL, rows), slice((h * 3 + r) * wide, (h * 3 + r + 1) * wide)) for r in THIRDS] for h in PAIR]
    third, half = rows // 3, cols // 2
    return [[(slice(r * third, (r + 1) * third), slice(h * half, (h + 1) * half)) for r in THIRDS] for h in PAIR]


class Gather:
    copies = 19

    def __init__(self, here, own, full, parts, sems, base, turned=NIL, rest=False):
        self.rest = rest
        self.here, self.own, self.full, self.parts = here, own, full, parts
        self.sems, self.base = sems, base
        self.turns = [TURNS[(r + turned) % 3] for r in THIRDS]

    def view(self, how, r):
        return self.full.at[self.here.at([(b, how.get(b, "m")) for b in BITS]) + self.parts[r]]

    def hop(self, p, r):
        d = self.turns[r]
        dst = self.view({b: "f" for b in d[:p]}, r)
        src = self.own.at[self.parts[r]] if p == NIL else dst
        return send(src, dst, self.sems, self.base + p * 3 + r, self.here.peer(d[p]))

    def across(self, p, r):
        d = self.turns[r]
        ref = self.view({**{b: "f" for b in d[:p]}, d[p]: "o"}, r)
        return send(ref, ref, self.sems, self.base + 9 + p * 3 + r, self.here.peer(1))

    def place(self):
        return self.full.at[self.here.at([(b, "m") for b in BITS])]

    def own_across(self):
        return send(self.own, self.place(), self.sems, self.base + 18, self.here.peer(1))

    def keep(self):
        return pltpu.make_async_copy(self.own, self.place(), self.sems.at[2, self.base])

    def begin(self):
        for r in THIRDS:
            self.hop(NIL, r).start()
        if not self.rest:
            self.keep().start()
            self.own_across().start()

    def onward(self, p):
        if p == NIL and not self.rest:
            self.keep().wait()
        for r in THIRDS:
            self.hop(p, r).wait_recv()
            if p < 2:
                self.hop(p + 1, r).start()
            self.across(p, r).start()

    def arrived(self):
        for p in THIRDS:
            for r in THIRDS:
                self.across(p, r).wait_recv()
        if not self.rest:
            self.own_across().wait_recv()

    def finish(self):
        for p in THIRDS:
            for r in THIRDS:
                self.hop(p, r).wait_send()
                self.across(p, r).wait_send()
        if not self.rest:
            self.own_across().wait_send()


def cuts(widths, lead):
    out, at = [], NIL
    for w in widths:
        out.append((slice(None),) * lead + (slice(at, at + w),))
        at += w
    return out


class Scatter:
    peers = AXES
    n_out = 1

    def __init__(self, sums, number, lag=0.0, halves=(NIL, 1), ready=None, shape=None):
        self.array, self.number, self.halves = sums, number, halves
        self.rows, self.cols = shape or sums.shape[4:]
        self.lag, self.ready = lag, ready
        self.n_in = NIL if ready else 1

    def inputs(self):
        return [] if self.ready else [(self.array, ANY)]

    def outputs(self):
        spec = pl.BlockSpec((self.rows, self.width()), lambda *_: (NIL, NIL), pipeline_mode=pl.Buffered(1))
        return [(jax.ShapeDtypeStruct((self.rows, self.width()), BF16), spec)]

    def width(self):
        return self.cols * len(self.halves) // 2

    def scratch(self):
        r, c = pieces(self.rows, self.cols)[NIL][NIL]
        r, c = r.stop - r.start, c.stop - c.start
        legs = [pltpu.VMEM((3 * len(self.halves), *lead, r, c), BF16) for lead in ((2, 2), (2,), ())]
        return [pltpu.VMEM((2, 2, 2, self.rows, self.width()), F32), *legs, *legs, pltpu.SemaphoreType.DMA((2, 18)), pltpu.SemaphoreType.DMA]

    def events(self, here, ins, outs, scratch):
        (out,) = outs
        held, *legs, wire, local = scratch
        self.held = held
        going, coming = legs[:3], legs[3:]
        parts = pieces(self.rows, self.cols)
        if not self.ready:
            sums = ins[NIL]
        if len(self.halves) == 1:
            sums = sums.at[:, :, :, :, :, pl.ds(self.halves[NIL] * self.width(), self.width())]
        load = None if self.ready else pltpu.make_async_copy(sums.at[self.number], held, local)

        def place(order, picks):
            where = dict(zip(order, picks, strict=True))
            return tuple(where[b] for b in AXES)

        def hop(p, h, r):
            q = h * 3 + r
            return send(going[p].at[q], coming[p].at[q], wire, p * 6 + q, here.peer(TURNS[r][p]))

        count = len(self.halves)

        def begin():
            load.start()

        def first(h):
            if h == NIL and load:
                load.wait()
            for r in THIRDS:
                d, q = TURNS[r], h * 3 + r
                for i in PAIR:
                    for j in PAIR:
                        going[NIL][q, i, j] = held[place(d, (1 - here.bit[d[NIL]], i, j)) + parts[h][r]].astype(BF16)
                hop(NIL, h, r).start()

        def onward(p, h):
            for r in THIRDS:
                d, q = TURNS[r], h * 3 + r
                mine = [here.bit[b] for b in d]
                hop(p, h, r).wait_recv()
                if p == NIL:
                    for j in PAIR:
                        at = place(d, (mine[NIL], 1 - mine[1], j)) + parts[h][r]
                        going[1][q, j] = (held[at] + coming[NIL][q, 1 - mine[1], j].astype(F32)).astype(BF16)
                    hop(1, h, r).start()
                    for j in PAIR:
                        at = place(d, (mine[NIL], mine[1], j)) + parts[h][r]
                        held[at] = held[at] + coming[NIL][q, mine[1], j].astype(F32)
                elif p == 1:
                    at = place(d, (mine[NIL], mine[1], 1 - mine[2])) + parts[h][r]
                    going[2][q] = (held[at] + coming[1][q, 1 - mine[2]].astype(F32)).astype(BF16)
                    hop(2, h, r).start()
                    at = place(d, mine) + parts[h][r]
                    held[at] = held[at] + coming[1][q, mine[2]].astype(F32)
                else:
                    at = place(d, mine) + parts[h][r]
                    out[parts[h][r]] = (held[at] + coming[2][q].astype(F32)).astype(BF16)

        def finish():
            for p in THIRDS:
                for h in range(count):
                    for r in THIRDS:
                        hop(p, h, r).wait_send()

        times = {(NIL, NIL): 12.0, (NIL, 1): 19.0, (1, NIL): 23.0, (1, 1): 26.5, (2, NIL): 28.5, (2, 1): 30.0}
        if count == 1:
            times = {(NIL, NIL): 12.0, (1, NIL): 17.5, (2, NIL): 21.0}
        if self.ready:
            out_events = [(step, functools.partial(first, h)) for h, step in enumerate(self.ready)]
        else:
            out_events = [(self.lag, begin)] + [(self.lag + HOP_US + h / 2, functools.partial(first, h)) for h in range(count)]
        for (p, h), t in times.items():
            out_events.append((self.lag + t, functools.partial(onward, p, h)))
        out_events.append((1e9, finish))
        return out_events


class Total:
    peers = "all"
    n_out = 1

    def __init__(self, blocks):
        self.blocks = blocks
        self.n_in = len(blocks)

    def inputs(self):
        return [whole(b) for b in self.blocks]

    def outputs(self):
        return [(jax.ShapeDtypeStruct((8, 128), F32), pl.BlockSpec((8, 128), lambda *_: (NIL, NIL)))]

    def scratch(self):
        return [pltpu.VMEM((16, 8, 128), F32), pltpu.SemaphoreType.DMA((2, 16))]

    def run(self, here, ins, outs, scratch, lasts):
        (all_sums, sems), (out,) = scratch, outs

        def squares(ref):
            rows, cols = ref.shape

            def step(i, acc):
                g = ref[pl.ds(pl.multiple_of(i * 16, 16), 16), :].astype(F32)
                g = g * g
                return acc + sum(g[:, k * 128 : (k + 1) * 128] for k in range(cols // 128))

            s = lax.fori_loop(NIL, rows // 16, step, jnp.zeros((16, 128), F32))
            return s[:8] + s[8:]

        total = sum(squares(ref) for ref in (*ins, *lasts))
        all_sums[here.me] = total
        copies = []
        for k in range(1, 16):
            to = lax.rem(here.me + k, 16)
            copies.append(send(all_sums.at[here.me], all_sums.at[here.me], sems, k, {"dp": to}))
        for c in copies:
            c.start()
        for c in copies:
            c.wait()
        total = all_sums[NIL]
        for k in range(1, 16):
            total = total + all_sums[k]
        out[...] = jnp.full((8, 128), jnp.sum(total), F32)


def stage(cid, name, steps, step_us, body, ins, outs, scratch=(), own_peers=(), comms=(), total=None, flops=NIL):
    comms = list(comms)
    everyone = comms + ([total] if total else [])
    args = [*ins] + [x for c in everyone for x in c.inputs()]
    results = [*outs] + [x for c in everyone for x in c.outputs()]
    temps = [*scratch] + [x for c in everyone for x in c.scratch()]
    peers = sorted({b for c in comms for b in c.peers} | set(own_peers))

    def kernel(*refs):
        here = Here()
        i, o = refs[: len(args)], refs[len(args) : len(args) + len(results)]
        s = refs[len(args) + len(results) :]
        at = pl.program_id(NIL)

        def barrier():
            sem = pltpu.get_barrier_semaphore()
            if total:
                for k in range(1, 16):
                    pl.semaphore_signal(sem, inc=1, device_id={"dp": lax.rem(here.me + k, 16)}, device_id_type=MESH)
                pl.semaphore_wait(sem, 15)
            else:
                for b in peers:
                    pl.semaphore_signal(sem, inc=1, device_id=here.peer(b), device_id_type=MESH)
                pl.semaphore_wait(sem, len(peers))

        events, ni, no, ns = [], len(ins), len(outs), len(scratch)
        for c in comms:
            ci, co, cs = i[ni : ni + c.n_in], o[no : no + c.n_out], s[ns : ns + len(c.scratch())]
            ni, no, ns = ni + c.n_in, no + c.n_out, ns + len(c.scratch())
            events += c.events(here, ci, co, cs)
        events.sort(key=lambda e: e[NIL] * step_us if isinstance(e[NIL], int) else e[NIL])
        by_step = {}
        for t, fn in events:
            k = t if isinstance(t, int) else int(t / step_us + 0.8)
            by_step.setdefault(min(steps, k) if t < 1e9 else steps + 1, []).append(fn)

        def run(fns):
            for fn in fns:
                fn()

        @pl.when(at == NIL)
        def _():
            if peers or total:
                barrier()
            run(by_step.get(NIL, []))

        for k in range(1, steps):
            if k in by_step:
                pl.when(at == k)(functools.partial(run, by_step[k]))
        if body:
            body(here, at, i[: len(ins)], o[: len(outs)], s[: len(scratch)])

        @pl.when(at == steps - 1)
        def _():
            run(by_step.get(steps, []) + by_step.get(steps + 1, []))
            if total:
                total.run(here, i[ni:], o[no:], s[ns:], o[len(outs) : no])

    got = pl.pallas_call(
        kernel,
        grid=(steps,),
        in_specs=[spec for _, spec in args],
        out_specs=[spec for _, spec in results],
        out_shape=[shape for shape, _ in results],
        scratch_shapes=temps,
        compiler_params=pltpu.CompilerParams(
            collective_id=cid if (peers or total) else None, has_side_effects=bool(peers or total), vmem_limit_bytes=63 * 1024 * 1024
        ),
        name=name,
    )(*[a for a, _ in args])
    return got


def whole(array):
    return (array, pl.BlockSpec(array.shape, lambda *_: (NIL,) * array.ndim, pipeline_mode=pl.Buffered(1)))


def by_rows(array, height):
    return (array, pl.BlockSpec((height, array.shape[1]), lambda i: (i, NIL)))


def new(shape, dtype, block, index):
    return (jax.ShapeDtypeStruct(shape, dtype), pl.BlockSpec(block, index))


def mm(a, b):
    return lax.dot_general(a, b, (((1,), (NIL,)), ((), ())), preferred_element_type=F32)


def mm_nt(a, b):
    return lax.dot_general(a, b, (((1,), (1,)), ((), ())), preferred_element_type=F32)


def norm_of(wide):
    scale = lax.rsqrt(jnp.mean(wide * wide, -1, keepdims=True) + 1e-6)
    return (wide * scale).astype(BF16)


COL = lambda s: (NIL, s)
ROW = lambda i: (i, NIL)


def sigmoid(g):
    return 0.5 * jnp.tanh(0.5 * g) + 0.5


def by_core(blocks, out, cols):
    rows = out.shape[2]
    for k in range(out.shape[1]):
        for c in PAIR:
            at = (2 * k + c) * rows
            out[c, k, :, cols] = blocks[at : at + rows, :]


WIDE = SPAN
UNITS = FF // WIDE
KINDS = 2, D // 16
CHUNK = FF // 3
WIRE_GU, WIRE_D = 16.8, 8.4
HOP_US, EARLY_US = 2.5, 4.0
CUT_GU, CUT_D = (384, 384, SPAN), (512, 384, 384)
PLACES = (2, 2, 2, 2)


def all_rows(fn):
    count = TOKENS // SPAN // 2

    def turn(j, _):
        for i in range(count):
            fn(pl.ds(pl.multiple_of((j * count + i) * SPAN, SPAN), SPAN))
        return NIL

    lax.fori_loop(NIL, 2, turn, NIL)


def tile_of(gu, c, which, q):
    return gu[c, :, :, :, :, which, :, pl.ds(pl.multiple_of(q * WIDE, WIDE), WIDE)].reshape(D, WIDE)


def by_third(block, out, c):
    out[...] = jnp.concatenate([block[:, n * 192 + c * 64 : n * 192 + c * 64 + 64] for n in range(16)], axis=1)


def barrier_of(here, peers):
    sem = pltpu.get_barrier_semaphore()
    for b in peers:
        pl.semaphore_signal(sem, inc=1, device_id=here.peer(b), device_id_type=MESH)
    pl.semaphore_wait(sem, len(peers))


def schedule(at, steps, table):
    by_step = {}
    for k, fn in table:
        by_step.setdefault(k, []).append(fn)
    for k, fns in by_step.items():

        @pl.when(at == k)
        def _(fns=fns):
            for fn in fns:
                fn()


def wire_order(units):
    legs = [("b", NIL)]
    for n in range(len(units)):
        legs += [("b", n + 1), (NIL, n + 1) if n else (NIL, NIL)] if n else [("b", 1), (NIL, NIL), ("b", 2), (NIL, 1)]
        legs += [(1, n)]
    order, seen = [], set()
    for leg in legs + [(NIL, n) for n in range(len(units))]:
        if leg not in seen and leg[1] < len(units):
            seen.add(leg)
            order.append(leg)
    wire, done, out, last = 0.0, {}, [], 0.0
    for kind, n in order:
        length, unit = units[n]
        if kind == "b":
            out.append((last, unit.begin, unit))
            wire = max(wire, last) + length / 7
            done[NIL, n] = wire
        else:
            last = max(last, done[kind, n] + HOP_US)
            out.append((last, functools.partial(unit.onward, kind), unit))
            wire = max(wire, last) + length * (2, 4)[kind] / 7
            done[kind + 1, n] = wire
    for n, (_, unit) in enumerate(units):
        unit.ready = done[2, n] + 4.0
        out.append((done[2, n] + HOP_US, functools.partial(unit.onward, 2), unit))
    return sorted(out, key=lambda e: e[NIL])


def placed(events, lengths, due, early=EARLY_US):
    starts, now = [], 0.0
    for i, length in enumerate(lengths):
        now = max([now] + [unit.ready for step, unit in due if step == i])
        starts.append(now)
        now += length
    out = []
    for t, fn, unit in events:
        k = next((i for i, u in enumerate(starts) if u >= t - early), len(starts))
        out.append((min([k] + [step for step, one in due if one is unit]), fn))
    return out


def call(cid, name, kernel, steps, ins, outs, scratch):
    return pl.pallas_call(
        kernel,
        grid=(steps,),
        in_specs=[spec for _, spec in ins],
        out_specs=[spec for _, spec in outs],
        out_shape=[shape for shape, _ in outs],
        scratch_shapes=scratch,
        compiler_params=pltpu.CompilerParams(collective_id=cid, has_side_effects=True, vmem_limit_bytes=67043328),
        name=name,
    )(*[a for a, _ in ins])


def blocks_of(array, *index):
    lead = len(index)
    block = (1,) * lead + array.shape[lead:]
    rest = (NIL,) * (array.ndim - lead)
    return (array, pl.BlockSpec(block, lambda s: index + rest, pipeline_mode=pl.Buffered(1)))


N1 = 8
G1 = N1 + UNITS
D1 = G1 + 4
E1 = D1 + 8


def first_stage(cid, x, wg, wu, wd):
    def kernel(x, wg, wu, wg1, wu1, wd_own, wd1_own, a_t, g_out, u_out, act_t, wd_full, h_out, a1_out, a1_t, gu1_full, wd1_full, *scratch):
        a, gu_all, wd_all, act, gu_own, gu1_own, sems, local = scratch
        wd_own, wd1_own = wd_own.at[NIL], wd1_own.at[NIL]
        here, at = Here(), pl.program_id(NIL)

        @pl.when(at == NIL)
        def _():
            for k, own in enumerate((wg, wu)):
                block = own[NIL]
                for c in THIRDS:
                    by_third(block, gu_own.at[c, k], c)
            for k, own in enumerate((wg1, wu1)):
                by_third(own[NIL], gu1_own.at[k], NIL)

        n = Gather.copies
        units = [Gather(here, gu_own.at[c], gu_all.at[c], cuts(CUT_GU, 2), sems, c * n, c) for c in THIRDS]
        halves = pieces(D3, D)
        units += [Gather(here, wd_own, wd_all, halves[h], sems, (3 + h) * n, rest=h == 1) for h in PAIR]
        units += [Gather(here, gu1_own, gu1_full, cuts(CUT_GU, 2), sems, 5 * n)]
        units += [Gather(here, wd1_own, wd1_full, cuts(CUT_D, 1), sems, 6 * n, 2)]

        timed = [(WIRE_D if i == 6 else WIRE_D * 1.5 if i in (3, 4) else WIRE_GU, unit) for i, unit in enumerate(units)]
        lengths = [1.0] * N1 + [3.6] * UNITS + [5.0] * (D1 - G1) + [1.0] * N1
        due = [(N1, units[NIL]), (N1 + 4, units[1]), (N1 + 8, units[2]), (G1, units[3]), (G1 + 2, units[4])]
        events = placed(wire_order(timed), lengths, due)
        waits = [(k, unit.arrived) for k, unit in due]
        spill = pltpu.make_async_copy(wd_all, wd_full, local)

        schedule(at, E1, [(NIL, functools.partial(barrier_of, here, BITS))])
        schedule(at, E1, [e for e in events if e[NIL] < E1])
        schedule(at, E1, waits)

        @pl.when(at < N1)
        def _():
            normed = norm_of(x[...].astype(F32))
            a[pl.ds(pl.multiple_of(at * SPAN, SPAN), SPAN), :] = normed
            by_core(normed.T, a_t, slice(None))

        @pl.when((at >= N1) & (at < G1))
        def _():
            t = at - N1
            c, q = lax.div(t, 4), lax.rem(t, 4)
            def part(rows):
                g = mm(a[rows, :], tile_of(gu_all, c, NIL, q))
                u = mm(a[rows, :], tile_of(gu_all, c, 1, q))
                v = (g * sigmoid(g) * u).astype(BF16)
                g_out[rows, :] = g
                u_out[rows, :] = u
                act[t, rows, :] = v
                by_core(v.T, act_t, rows)

            all_rows(part)

        @pl.when((at >= G1) & (at < D1))
        def _():
            t = at - G1
            cols = pl.ds(pl.multiple_of(lax.div(t, 2) * 640, 128), 640)

            def part(i, _):
                rows = pl.ds(pl.multiple_of(lax.rem(t, 2) * 1024 + i * 512, 512), 512)
                y = jnp.zeros((512, 640), F32)
                for c in THIRDS:
                    left = jnp.concatenate([act[c * 4 + q, rows, :] for q in range(4)], axis=1)
                    y = y + mm(left, wd_all[:, :, :, :, c * 64 : (c + 1) * 64, cols].reshape(CHUNK, 640))
                a[rows, cols] = y.astype(BF16)
                return NIL

            lax.fori_loop(NIL, 2, part, NIL)

        @pl.when(at == D1)
        def _():
            spill.start()

        @pl.when(at >= D1)
        def _():
            h = x[...] + a[pl.ds(pl.multiple_of((at - D1) * SPAN, SPAN), SPAN), :]
            h_out[...] = h
            normed = norm_of(h.astype(F32))
            a1_out[...] = normed
            by_core(normed.T, a1_t, slice(None))

        @pl.when(at == E1 - 1)
        def _():
            for k, fn in events:
                if k >= E1:
                    fn()
            for unit in units[5:]:
                unit.arrived()
            for unit in units:
                unit.finish()
            spill.wait()

    D3 = FF // 16
    tile = lambda s: jnp.clip(s - N1, NIL, UNITS - 1)
    early = lambda s: jnp.minimum(s, N1 - 1)
    late = lambda s: jnp.maximum(s - D1, NIL)
    strip = (2, 8, D // 16, TOKENS)
    outs = [
        new(strip, BF16, (*strip[:3], SPAN), lambda s: (NIL, NIL, NIL, early(s))),
        new((TOKENS, FF), F32, (TOKENS, WIDE), lambda s: (NIL, tile(s))),
        new((TOKENS, FF), F32, (TOKENS, WIDE), lambda s: (NIL, tile(s))),
        new((2, 8, D3, TOKENS), BF16, (2, 2, 64, TOKENS), lambda s: (NIL, lax.rem(tile(s), 4), lax.div(tile(s), 4), NIL)),
        (jax.ShapeDtypeStruct((*PLACES, D3, D), BF16), ANY),
        new((TOKENS, D), BF16, (SPAN, D), lambda s: (late(s), NIL)),
        new((TOKENS, D), BF16, (SPAN, D), lambda s: (late(s), NIL)),
        new(strip, BF16, (*strip[:3], SPAN), lambda s: (NIL, NIL, NIL, late(s))),
        (jax.ShapeDtypeStruct((*PLACES, *KINDS, CHUNK), BF16), ANY),
        (jax.ShapeDtypeStruct((*PLACES, 64, D), BF16), ANY),
    ]
    ins = [(x, pl.BlockSpec((SPAN, D), lambda s: (jnp.where(s < D1, early(s), late(s)), NIL)))]
    ins += [blocks_of(wg, NIL), blocks_of(wu, NIL), blocks_of(wg, 1), blocks_of(wu, 1), blocks_of(wd, NIL)]
    ins += [(wd, pl.BlockSpec((1, 64, D), lambda s: (1, NIL, NIL), pipeline_mode=pl.Buffered(1)))]
    scratch = [
        pltpu.VMEM((TOKENS, D), BF16),
        pltpu.VMEM((3, *PLACES, *KINDS, CHUNK), BF16),
        pltpu.VMEM((*PLACES, D3, D), BF16),
        pltpu.VMEM((UNITS, TOKENS, WIDE), BF16),
        pltpu.VMEM((3, *KINDS, CHUNK), BF16),
        pltpu.VMEM((*KINDS, CHUNK), BF16),
        pltpu.SemaphoreType.DMA((3, 7 * Gather.copies)),
        pltpu.SemaphoreType.DMA,
    ]
    return call(cid, "first", kernel, E1, ins, outs, scratch)


def second_stage(cid, a, dy, wg, wu, wd, gu_first, wd_first):
    def kernel(a_in, dy_in, wg, wu, wd_own, gu_first, wd_first, dgu, act_t, gu_rest, *scratch):
        gu_all, wd_all, gu_own, a, dy, sems, local = scratch
        wd_own = wd_own.at[NIL]
        here, at = Here(), pl.program_id(NIL)

        @pl.when(at == NIL)
        def _():
            for k, own in enumerate((wg, wu)):
                block = own[NIL]
                for c in (1, 2):
                    by_third(block, gu_own.at[c - 1, k], c)

        n = Gather.copies
        units = []
        for c in (1, 2):
            units.append(Gather(here, gu_own.at[c - 1], gu_all.at[c], cuts(CUT_GU, 2), sems, len(units) * n, c))
            units.append(Gather(here, wd_own.at[pl.ds(c * 64, 64)], wd_all.at[c], cuts(CUT_D, 1), sems, len(units) * n, c + 2))
        timed = list(zip((WIRE_GU, WIRE_D) * 2, units, strict=True))
        due = [(4, units[NIL]), (4, units[1]), (8, units[2]), (8, units[3])]
        events = placed(wire_order(timed), [5.6] * UNITS, due, 2 * EARLY_US)
        moves = ((a_in, a), (gu_first, gu_all.at[NIL]), (dy_in, dy), (wd_first, wd_all.at[NIL]))
        loads = [pltpu.make_async_copy(src, dst, local.at[i]) for i, (src, dst) in enumerate(moves)]
        spills = [pltpu.make_async_copy(gu_all.at[c], gu_rest.at[c - 1], local.at[3 + c]) for c in (1, 2)]
        table = [(NIL, load.start) for load in loads] + [(NIL, functools.partial(barrier_of, here, BITS))]
        table += [e for e in events if e[NIL] < UNITS]
        table += [(NIL, load.wait) for load in loads]
        table += [(k, unit.arrived) for k, unit in due] + [(4, spills[NIL].start), (8, spills[1].start)]
        schedule(at, UNITS, table)

        c, q = lax.div(at, 4), lax.rem(at, 4)
        qx, qy = lax.div(q, 2), lax.rem(q, 2)
        def part(rows):
            g = mm(a[rows, :], tile_of(gu_all, c, NIL, q))
            u = mm(a[rows, :], tile_of(gu_all, c, 1, q))
            dact = mm_nt(dy[rows, :], wd_all[c, qx, qy].reshape(WIDE, D)).astype(BF16).astype(F32)
            s = sigmoid(g)
            silu = g * s
            by_core((silu * u).astype(BF16).T, act_t, rows)
            dgu[NIL, rows, :] = (dact * u * (s + silu * (1.0 - s))).astype(BF16)
            dgu[1, rows, :] = (dact * silu).astype(BF16)

        all_rows(part)

        @pl.when(at == UNITS - 1)
        def _():
            for unit in units:
                unit.finish()
            for s in spills:
                s.wait()

    outs = [
        new((2, TOKENS, FF), BF16, (2, TOKENS, WIDE), lambda s: (NIL, NIL, s)),
        new((2, 8, FF // 16, TOKENS), BF16, (2, 2, 64, TOKENS), lambda s: (NIL, lax.rem(s, 4), lax.div(s, 4), NIL)),
        (jax.ShapeDtypeStruct((2, *PLACES, *KINDS, CHUNK), BF16), ANY),
    ]
    ins = [(a, ANY), (dy, ANY), blocks_of(wg, 1), blocks_of(wu, 1), blocks_of(wd, 1), (gu_first, ANY), (wd_first, ANY)]
    scratch = [
        pltpu.VMEM((3, *PLACES, *KINDS, CHUNK), BF16),
        pltpu.VMEM((3, *PLACES, 64, D), BF16),
        pltpu.VMEM((2, *KINDS, CHUNK), BF16),
        *[pltpu.VMEM((TOKENS, D), BF16)] * 2,
        pltpu.SemaphoreType.DMA((3, 4 * Gather.copies)),
        pltpu.SemaphoreType.DMA((6,)),
    ]
    return call(cid, "second", kernel, UNITS, ins, outs, scratch)


def dact_stage(cid, dy, wd, g, u, comms):
    def body(here, at, ins, outs, scratch):
        dy, wd, g_in, u_in = ins
        def part(rows):
            dact = mm_nt(dy[rows, :], wd[...].reshape(WIDE, D)).astype(BF16).astype(F32)
            g, u = g_in[rows, :], u_in[rows, :]
            s = sigmoid(g)
            silu = g * s
            outs[NIL][NIL, rows, :] = (dact * u * (s + silu * (1.0 - s))).astype(BF16)
            outs[NIL][1, rows, :] = (dact * silu).astype(BF16)

        all_rows(part)

    outs = [new((2, TOKENS, FF), BF16, (2, TOKENS, WIDE), lambda s: (NIL, NIL, s))]
    tile = pl.BlockSpec((TOKENS, WIDE), COL)
    ins = [whole(dy), (wd, pl.BlockSpec((4, 64, D), lambda s: (lax.rem(s, 4), lax.div(s, 4), NIL))), (g, tile), (u, tile)]
    return stage(cid, "dact", UNITS, 2.5, body, ins, outs, comms=comms)


def dinput_stage(cid, dgu, gu_first, gu_rest, h, dy, comms):
    def body(here, at, ins, outs, scratch):
        dgu, gu_first, gu_rest, h, dy = ins
        back = []
        for k in PAIR:
            total = mm_nt(dgu[k, :, :CHUNK], gu_first[:, :, :, :, k].reshape(D, CHUNK))
            for c in range(1, 3):
                total += mm_nt(dgu[k, :, c * CHUNK : (c + 1) * CHUNK], gu_rest[c - 1, :, :, :, :, k].reshape(D, CHUNK))
            back.append(total.astype(BF16))
        da = (back[NIL] + back[1]).astype(F32)
        wide = h[...].astype(F32)
        scale = lax.rsqrt(jnp.mean(wide * wide, -1, keepdims=True) + 1e-6)
        along = jnp.mean(da * wide, -1, keepdims=True)
        dh = da * scale - wide * (scale * scale * scale * along)
        outs[NIL][...] = dy[...] + dh.astype(BF16)

    outs = [new((TOKENS, D), BF16, (SPAN, D), ROW)]
    ins = [(dgu, pl.BlockSpec((2, SPAN, FF), lambda i: (NIL, i, NIL))), whole(gu_first), whole(gu_rest), by_rows(h, SPAN), by_rows(dy, SPAN)]
    return stage(cid, "dinput", 8, 5.2, body, ins, outs, comms=comms)


def dw_stage(cid, left, right, comms, into=(), total=None):
    rows, (count, _, n) = left.shape[2], right.shape
    width = 512 if n == FF else SPAN
    per = n // width
    turn = 2 * per

    def body(here, at, ins, outs, scratch):
        left_in, right = ins
        left, going, coming, sems, local = scratch
        core = here.bit[1]
        step = 4 if rows == 80 else 2
        matrix, place = lax.div(at, turn), lax.rem(at, turn)

        def load(c):
            return pltpu.make_async_copy(left_in.at[c], left.at[c], local.at[c])

        @pl.when(at == NIL)
        def _():
            load(1 - core).start()
            load(core).start()
            load(1 - core).wait()

        @pl.when(at == per)
        def _():
            load(core).wait()

        def swap(t):
            one = matrix * per + t
            return send(going.at[t], coming.at[one], sems, one, here.peer(1))

        @pl.when(place < per)
        def _():
            for k in range(NIL, 8, step):
                a = left[1 - core, k : k + step].reshape(step * rows, TOKENS)
                going[place, k : k + step] = mm(a, right[NIL]).astype(BF16).reshape(step, rows, width)
            swap(place).start()

        def own(put):
            t = place - per
            swap(t).wait()
            for k in range(NIL, 8, step):
                a = left[core, k : k + step].reshape(step * rows, TOKENS)
                got = mm(a, right[NIL]).reshape(step, rows, width)
                for i in range(step):
                    where = (k + i) // 4, (k + i) // 2 % 2, (k + i) % 2
                    put(where, t, got[i] + coming[matrix * per + t, k + i].astype(F32))

        def put_out(where, t, value):
            outs[NIL][(NIL, *where)] = value

        if into:
            for m, scatter in enumerate(into):

                def put_held(where, t, value, held=scatter.held):
                    held[(*where, slice(None), pl.ds(pl.multiple_of(t * width, width), width))] = value

                pl.when((place >= per) & (matrix == m))(functools.partial(own, put_held))
        else:
            pl.when(place >= per)(functools.partial(own, put_out))

    def source(s):
        return (lax.div(s, turn), NIL, lax.rem(lax.rem(s, turn), per))

    def back(s):
        return (lax.div(s, turn), NIL, NIL, NIL, NIL, jnp.maximum(lax.rem(s, turn) - per, NIL))

    outs = [] if into else [new((count, 2, 2, 2, rows, n), F32, (1, 2, 2, 2, rows, width), back)]
    scratch = [pltpu.VMEM(left.shape, BF16), pltpu.VMEM((per, 8, rows, width), BF16), pltpu.VMEM((count * per, 8, rows, width), BF16)]
    scratch += [pltpu.SemaphoreType.DMA((2, count * per)), pltpu.SemaphoreType.DMA((2,))]
    ins = [(left, ANY), (right, pl.BlockSpec((1, TOKENS, width), source))]
    steps = count * turn
    return stage(cid, "dw", steps, count * 21.0 / steps, body, ins, outs, scratch, own_peers=(1,), comms=[*comms, *into], total=total)


def update_stage(weights, moments, seconds, sums, squares):
    steps = 5
    flat = [piece for pair in sums for layer in pair for piece in layer]
    count = 16 * sum(w.size for w in weights)

    def kernel(*refs):
        squares, ws, ms, vs = refs[NIL], refs[1:4], refs[4:7], refs[7:10]
        pieces_in, outs = list(refs[10 : 10 + len(flat)]), refs[10 + len(flat) :]
        factor = jnp.minimum(1.0, 0.5 * lax.rsqrt(squares[...] / count + 1e-30))[:1, :1]
        for i in THIRDS:
            for n in PAIR:
                taken = [pieces_in.pop(NIL) for _ in sums[i][n]]
                g = jnp.concatenate([r[...] for r in taken], axis=1) if len(taken) > 1 else taken[NIL][...]
                if i < 2:
                    at = [c * CHUNK + k * 64 for k in range(16) for c in THIRDS]
                    g = jnp.concatenate([g[:, u : u + 64] for u in at], axis=1)
                g = g.astype(F32) * factor
                m = 0.9 * ms[i][n] + 0.1 * g
                v = 0.95 * vs[i][n] + 0.05 * g * g
                w = ws[i][n].astype(F32)
                outs[i][n] = (w - 0.02 * (m * lax.rsqrt(v + 1e-8) + 0.1 * w)).astype(BF16)
                outs[3 + i][n] = m
                outs[6 + i][n] = v

    def spec(array):
        lead = array.ndim - 2
        rows, cols = array.shape[lead:]
        height = 16 if rows == D // 16 else 48
        last = rows // height - 1
        return pl.BlockSpec((2,) * lead + (height, cols), lambda s: (NIL,) * lead + (jnp.minimum(s, last), NIL))

    args = [*weights, *moments, *seconds, *flat]
    like = [*weights, *moments, *seconds]
    return pl.pallas_call(
        kernel,
        grid=(steps,),
        in_specs=[pl.BlockSpec((8, 128), lambda s: (NIL, NIL))] + [spec(a) for a in args],
        out_specs=[spec(a) for a in like],
        out_shape=[jax.ShapeDtypeStruct(a.shape, a.dtype) for a in like],
        compiler_params=pltpu.CompilerParams(vmem_limit_bytes=60 * 1024 * 1024),
        name="update",
    )(squares, *args)


def solution(mesh):
    def step(x, dy, *arrays):
        weights, m, v = (arrays[i : i + 3] for i in (NIL, 3, 6))
        wg, wu, wd = weights
        x, dy = x[NIL], dy[NIL]
        a0_t, g0, u0, act0_t, wd0, h1, a1, a1_t, gu1_first, wd1_first = first_stage(NIL, x, wg, wu, wd)
        dgu1, act1_t, gu1_rest = second_stage(1, a1, dy, wg, wu, wd, gu1_first, wd1_first)
        (s_d1,) = dw_stage(9, act1_t, dy[None], [])
        s_1, r_d1 = dw_stage(2, a1_t, dgu1, [Scatter(s_d1, NIL)])
        dh1, r_g1 = dinput_stage(3, dgu1, gu1_first, gu1_rest, h1, dy, [Scatter(s_1, NIL)])
        s_d0, r_u1a = dw_stage(4, act0_t, dh1[None], [Scatter(s_1, 1, halves=(NIL,))])
        early = [Scatter(s_1, 1, halves=(1,)), Scatter(s_d0, NIL, 11.0, halves=(NIL,))]
        dgu0, r_u1b, r_d0a = dact_stage(5, dh1, wd0.reshape(16, FF // 16, D), g0, u0, early)
        block = (D // 16, FF)
        late = [Scatter(None, NIL, 14.0, ready=(9, 12), shape=block), Scatter(None, NIL, 40.0, ready=(21, 24), shape=block)]
        total = Total([r_d1, r_g1, r_u1a, r_u1b, r_d0a])
        r_d0b, r_g0, r_u0, squares = dw_stage(6, a0_t, dgu0, [Scatter(s_d0, NIL, halves=(1,))], late, total)
        sums = (((r_g0,), (r_g1,)), ((r_u0,), (r_u1a, r_u1b)), ((r_d0a, r_d0b), (r_d1,)))
        return tuple(update_stage(weights, m, v, sums, squares))

    states, cut = P(("rep", "dp"), None, None), P(None, "dp", None)
    return jax.shard_map(
        step,
        mesh=mesh,
        in_specs=(states, states) + (cut,) * 9,
        out_specs=(P("rep", "dp", None),) * 9,
        check_vma=False,
    )
```
